256 devices in a mesh: tm: 8 (over z_hi, x), gx: 8 (over z_lo, core), gy: 4 (over y).
Axes of the slice: x: 4, y: 4, z: 8 (z_hi: 2, z_lo: 4; z = z_hi * 4 + z_lo), core: 2. Of those that a mesh axis runs over, the one named last changes fastest.
Arguments:
- increment: float32 [8, 137, 128, 512], P('tm', None, 'gx', 'gy'), may hold values from -6 to 6
- dual_state: float32 [8, 137, 128, 512], P('tm', None, 'gx', 'gy'), may hold values from -6 to 6
- forcing: float32 [8, 137, 128, 512], P('tm', None, 'gx', 'gy'), may hold values from -6 to 6
- gradient: float32 [8, 137, 128, 512], P('tm', None, 'gx', 'gy'), may hold values from -3 to 3
- courant_x: float32 [8, 137, 128, 512], P('tm', None, 'gx', 'gy'), may hold values from 0.05 to 0.3
- courant_y: float32 [8, 137, 128, 512], P('tm', None, 'gx', 'gy'), may hold values from 0.05 to 0.3
- error_var: float32 [8, 137, 128, 512], P('tm', None, 'gx', 'gy'), may hold values from 0.2 to 2
- obs_weight: float32 [8, 137, 128, 512], P('tm', None, 'gx', 'gy'), may hold values from 0.2 to 2
- diffusion: float32 [137], replicated, may hold values from 0.02 to 0.1
- level_mix: float32 [137, 137], replicated, may hold values from -0.5 to 0.8
Outputs:
- dual_next: float32 [8, 137, 128, 512], P('tm', None, 'gx', 'gy')
- increment_next: float32 [8, 137, 128, 512], P('tm', None, 'gx', 'gy')
The draws below stay inside these ranges and needn't reach their ends.
All inputs are finite; a program needn't handle non-finite values.
Results may differ from the reference program's by a relative error of at most 0.0001.
Values sent between devices are 32-bit elements; how exact they have to be, the bound alone decides.
A program may use at most 128 MiB of HBM per device.

```python
import math
import jax
import jax.numpy as jnp
from jax import lax

LEVELS = 137
STEPS = 3
SUBWIN = 8
NX = 128
NY = 512


def coherent_field(key):
    level_place = ((jnp.arange(LEVELS, dtype=jnp.float32) + 0.5) / LEVELS)[None, :, None, None]
    along_x = (jnp.arange(NX, dtype=jnp.float32) / NX)[None, None, :, None]
    along_y = (jnp.arange(NY, dtype=jnp.float32) / NY)[None, None, None, :]
    window_place = jnp.arange(SUBWIN, dtype=jnp.float32) / max(SUBWIN - 1, 1)
    window_scale = (0.6 + 0.4 * window_place)[:, None, None, None]
    summed = jnp.zeros((SUBWIN, LEVELS, NX, NY), jnp.float32)
    for mode in range(3):
        mode_key = jax.random.fold_in(key, 31 + mode)
        mode_keys = jax.random.split(mode_key, 6)
        wave_x = jax.random.randint(mode_keys[0], (), 1, 3).astype(jnp.float32)
        wave_y = jax.random.randint(mode_keys[1], (), 1, 3).astype(jnp.float32)
        wave_level = jax.random.randint(mode_keys[2], (), 0, 3).astype(jnp.float32)
        phases = jax.random.uniform(mode_keys[3], (3,), jnp.float32, -math.pi, math.pi)
        strength = jax.random.uniform(mode_keys[4], (), jnp.float32, 0.6, 1.0)
        jitter = 1.0 + 0.1 * jax.random.uniform(mode_keys[5], (SUBWIN, 1, 1, 1), jnp.float32, -1.0, 1.0)
        pattern = jnp.cos(2.0 * math.pi * wave_x * along_x + phases[0])
        pattern = pattern * jnp.cos(2.0 * math.pi * wave_y * along_y + phases[1])
        pattern = pattern * jnp.cos(math.pi * wave_level * level_place + phases[2])
        summed = summed + strength * jitter * pattern
    rough_key = jax.random.fold_in(key, 97)
    smooth = 1.4 * summed
    roughness = 0.5 * jnp.clip(jax.random.normal(rough_key, (SUBWIN, LEVELS, NX, NY), jnp.float32), -2.5, 2.5)
    return window_scale * smooth + roughness


def draw_increment(key, part):
    return coherent_field(jax.random.fold_in(key, 101))


def draw_dual_state(key, part):
    return coherent_field(jax.random.fold_in(key, 202))


def draw_forcing(key, part):
    normal_part = 0.5 * jnp.clip(jax.random.normal(key, (SUBWIN, LEVELS, NX, NY), jnp.float32), -4.0, 4.0)
    growth = 1.0 + 2.0 * jnp.arange(SUBWIN, dtype=jnp.float32) / max(SUBWIN - 1, 1)
    growth = growth[:, None, None, None]
    return normal_part * growth


def draw_level_mix(key, part):
    key_diag = jax.random.fold_in(key, 11)
    key_coupling = jax.random.fold_in(key, 23)
    diagonal = jax.random.uniform(key_diag, (LEVELS,), jnp.float32, 0.5, 0.8)
    coupling = jnp.clip(jax.random.normal(key_coupling, (LEVELS, LEVELS), jnp.float32), -6.0, 6.0) * (0.3 / math.sqrt(LEVELS))
    coupling = coupling * (1.0 - jnp.eye(LEVELS, dtype=jnp.float32))
    return coupling + jnp.diag(diagonal)


def block_levels(key, shape, cuts, least, high):
    loudness, own = 1.0, jax.random.fold_in(key, 6)
    for position, blocks in cuts:
        draws = jnp.exp(jax.random.uniform(jax.random.fold_in(own, position), (blocks,), jnp.float32, least / len(cuts), high / len(cuts)))
        loudness = loudness * jnp.repeat(draws, shape[position] // blocks).reshape([-1 if axis == position else 1 for axis in range(len(shape))])
    return loudness


def bell_draw(stream_key, dims, width, limit, cuts=(), kind=jnp.bfloat16):
    entries = jax.random.normal(stream_key, dims, jnp.float32) * width
    if len(cuts) > 0:
        entries = block_levels(stream_key, dims, cuts, -0.22, 0.18) * entries
    return jnp.clip(entries, min=-limit, max=limit).astype(kind)


def setup_inputs(seed: int = 0) -> dict:
    arg_keys = jax.random.split(jax.random.key(seed), 11)
    increment = draw_increment(jax.random.fold_in(arg_keys[10], 71), 0)
    dual_state = draw_dual_state(jax.random.fold_in(arg_keys[10], 71), 0)
    forcing = draw_forcing(jax.random.fold_in(arg_keys[10], 71), 0)
    gradient = bell_draw(arg_keys[3], (SUBWIN, LEVELS, NX, NY), 0.5, 3.0, ((0, 8), (2, 8), (3, 4)), jnp.float32)
    courant_x = jnp.clip(0.05 + 0.25 * jax.random.uniform(arg_keys[4], (SUBWIN, LEVELS, NX, NY), jnp.float32) ** block_levels(arg_keys[4], (SUBWIN, LEVELS, NX, NY), ((0, 8), (2, 8), (3, 4)), -0.2, 0.2), 0.05, 0.3)
    courant_y = jnp.clip(0.05 + 0.25 * jax.random.uniform(arg_keys[5], (SUBWIN, LEVELS, NX, NY), jnp.float32) ** block_levels(arg_keys[5], (SUBWIN, LEVELS, NX, NY), ((0, 8), (2, 8), (3, 4)), -0.2, 0.2), 0.05, 0.3)
    error_var = jnp.clip(jnp.exp(math.log(2.0) - 2.3025851 * jax.random.uniform(arg_keys[6], (SUBWIN, LEVELS, NX, NY), jnp.float32) ** block_levels(arg_keys[6], (SUBWIN, LEVELS, NX, NY), ((0, 8), (2, 8), (3, 4)), -0.2, 0.2)), 0.2, 2.0)
    obs_weight = jnp.clip(jnp.exp(math.log(2.0) - 2.3025851 * jax.random.uniform(arg_keys[7], (SUBWIN, LEVELS, NX, NY), jnp.float32) ** block_levels(arg_keys[7], (SUBWIN, LEVELS, NX, NY), ((0, 8), (2, 8), (3, 4)), -0.2, 0.2)), 0.2, 2.0)
    diffusion = jnp.clip(jnp.exp(jax.random.uniform(arg_keys[8], (LEVELS,), jnp.float32, math.log(0.02), math.log(0.1))), 0.02, 0.1)
    level_mix = draw_level_mix(jax.random.fold_in(arg_keys[10], 71), 0)
    return dict(increment=increment, dual_state=dual_state, forcing=forcing, gradient=gradient, courant_x=courant_x, courant_y=courant_y, error_var=error_var, obs_weight=obs_weight, diffusion=diffusion, level_mix=level_mix)


def apply_levels(matrix, current):
    return jnp.einsum('lm,mxy->lxy', matrix, current, precision=lax.Precision.HIGHEST)

def neighbours(current):
    padded = jnp.pad(current, ((0, 0), (1, 1), (1, 1)))
    return (padded[:, :-2, 1:-1], padded[:, 2:, 1:-1], padded[:, 1:-1, :-2], padded[:, 1:-1, 2:])

def tangent_step(current, courant_x, courant_y, lower_x, lower_y, spread, level_mix):
    minus_x, plus_x, minus_y, plus_y = neighbours(current)
    advected = (1.0 - courant_x - courant_y - 4.0 * spread) * current + lower_x * minus_x + lower_y * minus_y
    advected = advected + spread * (minus_x + plus_x + minus_y + plus_y)
    return apply_levels(level_mix, advected)

def adjoint_step(current, courant_x, courant_y, spread, level_mix):
    mixed_back = apply_levels(level_mix.T, current)
    minus_x, plus_x, minus_y, plus_y = neighbours(mixed_back)
    result = (1.0 - courant_x - courant_y - 4.0 * spread) * mixed_back + courant_x * plus_x + courant_y * plus_y
    return result + spread * (minus_x + plus_x + minus_y + plus_y)

def reference(increment, dual_state, forcing, gradient, courant_x, courant_y, error_var, obs_weight, diffusion, level_mix):
    spread = diffusion[:, None, None]
    windows = increment.shape[0]
    end_states = []
    back_states = []
    for window in range(windows):
        flow_x = courant_x[window]
        flow_y = courant_y[window]
        lower_x = jnp.pad(flow_x, ((0, 0), (1, 0), (0, 0)))[:, :-1, :]
        lower_y = jnp.pad(flow_y, ((0, 0), (0, 0), (1, 0)))[:, :, :-1]
        forward_state = increment[window]
        for substep in range(STEPS):
            forward_state = tangent_step(forward_state, flow_x, flow_y, lower_x, lower_y, spread, level_mix)
        end_states.append(forward_state)
        if window + 1 < windows:
            adjoint_state = dual_state[window + 1]
        else:
            adjoint_state = jnp.zeros_like(dual_state[0])
        for substep in range(STEPS):
            adjoint_state = adjoint_step(adjoint_state, flow_x, flow_y, spread, level_mix)
        back_states.append(adjoint_state)
    earlier_end = jnp.stack([jnp.zeros_like(increment[0])] + end_states[:-1])
    back_all = jnp.stack(back_states)
    residual_dual = forcing - error_var * dual_state - increment + earlier_end
    residual_incr = gradient - obs_weight * increment - dual_state + back_all
    global_sum = jnp.sum(residual_dual * residual_dual) + jnp.sum(residual_incr * residual_incr)
    cell_count = 2 * residual_dual.size
    root_mean = jnp.sqrt(global_sum / cell_count + 1e-06)
    step_scale = jnp.minimum(1.0, 0.5 / root_mean)
    return (dual_state + step_scale * residual_dual, increment + step_scale * residual_incr)
```

```python
import functools

import jax
import jax.numpy as jnp
from jax import lax
from jax.experimental import pallas as pl
from jax.experimental.pallas import tpu as pltpu
from jax.sharding import PartitionSpec as P

STEPS = 3
F32 = jnp.float32
BF16 = jnp.bfloat16
LANES = 128
MESH = pl.DeviceIdType.MESH


class Sizes:
    def __init__(self, mesh, levels, planes):
        self.tm, self.gx, self.gy = (mesh.shape[a] for a in ("tm", "gx", "gy"))
        self.xs = self.tm // 2
        self.levels = levels
        self.planes = planes
        self.rows = -(-levels // 16) * 16
        self.depth = 3 * self.rows


def kernel(
    sz,
    inc_h, dual_h, forc_h, grad_h, cx_h, cy_h, ev_h, ob_h, diff_r, mix_r,
    out_dual, out_incr,
    inc, dual, forc, grad, cx, cy, ev, ob,
    later, earlier, end,
    ca, cb, cc, sb, state, packs, halos, xsend, bpack, bhalo, asend,
    wcat, tb, stage_a, stage_b,
    load_sem, store_sem, d_send, d_recv, e_send, e_recv, h_send, h_recv, r_send, p_send, p_recv,
):
    NP, R, L = sz.planes, sz.rows, sz.levels
    XS = sz.xs
    t, g, y = (lax.axis_index(a) for a in ("tm", "gx", "gy"))
    xc, zh = lax.rem(t, XS), lax.div(t, XS)
    core, zl = lax.rem(g, 2), lax.div(g, 2)
    last_t = sz.tm - 1
    zchips = sz.gx // 2
    half = NP // 2

    def rdma(src, dst, ssem, rsem, **where):
        return pltpu.make_async_remote_copy(
            src_ref=src, dst_ref=dst, send_sem=ssem, recv_sem=rsem, device_id=where, device_id_type=MESH
        )

    def wait(ref, sem):
        pltpu.make_async_copy(ref, ref, sem).wait()

    hbm = (inc_h, cx_h, cy_h, dual_h, forc_h, ev_h, ob_h, grad_h)
    local = (inc, cx, cy, dual, forc, ev, ob, grad)
    valid = pl.ds(0, L)

    def load(i, x):
        return pltpu.make_async_copy(hbm[i].at[0, :, x, :], local[i].at[x, valid, :], load_sem.at[i, x])

    for x in range(NP):
        for i in range(3):
            load(i, x).start()
    for i in range(3, 8):
        for x in range(NP):
            load(i, x).start()

    barrier = pltpu.get_barrier_semaphore()
    group_a = [(dx, dy, dc) for dx in range(XS) for dy in range(sz.gy) for dc in range(2)][1:]
    group_b = [(dh, dl) for dh in range(2) for dl in range(zchips)][1:]

    def peer_a(dx, dy, dc):
        return {
            "tm": zh * XS + lax.rem(xc + dx, XS),
            "gy": lax.rem(y + dy, sz.gy),
            "gx": zl * 2 + lax.rem(core + dc, 2),
        }

    def peer_b(dh, dl):
        return {"tm": lax.rem(zh + dh, 2) * XS + xc, "gx": lax.rem(zl + dl, zchips) * 2 + core}

    def greet(where):
        pl.semaphore_signal(barrier, inc=1, device_id=where, device_id_type=MESH)

    for p in group_a:
        greet(peer_a(*p))
    for p in group_b:
        greet(peer_b(*p))
    outward = jnp.where(core == 0, g - 1, g + 1)
    has_out = (outward >= 0) & (outward < sz.gx)

    @pl.when(has_out)
    def _():
        greet({"gx": outward})

    across = (t == XS - 1) | (t == XS)

    @pl.when(across)
    def _():
        greet({"tm": 2 * XS - 1 - t})

    lane = lax.broadcasted_iota(jnp.int32, (8, LANES), 1)

    def at_lane(k, n):
        return jnp.broadcast_to((lane == k % LANES)[None], (n // 8, 8, LANES)).reshape(n, LANES)

    chunks = [(r, min(48, R - r)) for r in range(0, R, 48)]

    lifted = jnp.concatenate([diff_r[...], jnp.zeros((1, 2 * LANES - L), F32)], axis=1)
    turned = jnp.broadcast_to(lifted, (LANES, 2 * LANES)).T
    sb[...] = turned[:R]

    def widen(m):
        high = m.astype(BF16).astype(F32)
        low = m - high
        tail = jnp.where(lane[:1] < R - LANES, high[:, LANES:], 0.0)
        tail_low = jnp.where(lane[:1] < R - LANES, low[:, LANES:], 0.0)
        k = R - LANES
        tails = tail + pltpu.roll(tail, k, 1) + pltpu.roll(tail_low, 2 * k, 1)
        whole = jnp.concatenate([high[:, :LANES], high[:, :LANES], low[:, :LANES], tails], axis=1)
        return whole[:, : sz.depth].astype(BF16)

    mix = jnp.concatenate([mix_r[...], jnp.zeros((L, 2 * LANES - L), F32)], axis=1)
    mix = jnp.concatenate([mix, jnp.zeros((2 * LANES - L, 2 * LANES), F32)], axis=0)
    wcat[0] = widen(mix[:R])
    wcat[1] = widen(mix.T[:R])

    row = lax.broadcasted_iota(jnp.int32, (R, LANES), 0)

    def clean(v, r, n):
        return v if r + n <= L else jnp.where(row[r : r + n] < L, v, 0.0)

    @pl.when(g == 0)
    def _():
        for k in range(2 * STEPS):
            state[k, 0] = jnp.zeros((R, LANES), F32)
        ca[0] = jnp.zeros((R, LANES), F32)

    @pl.when(g == sz.gx - 1)
    def _():
        for k in range(2 * STEPS):
            state[k, NP + 1] = jnp.zeros((R, LANES), F32)

    @pl.when(y == 0)
    def _():
        for k in range(2 * STEPS):
            halos[k, 0] = jnp.zeros((R, LANES), F32)
        bhalo[...] = jnp.zeros((R, LANES), F32)

    @pl.when(y == sz.gy - 1)
    def _():
        for k in range(2 * STEPS):
            halos[k, 1] = jnp.zeros((R, LANES), F32)

    def keep(k, x, r, n, v):
        rows = pl.ds(r, n)
        state[k, x + 1, rows, :] = v
        pltpu.store(packs.at[k, 0, rows, :], v, mask=at_lane(x - 1, n))
        pltpu.store(packs.at[k, 1, rows, :], v, mask=at_lane(x, n))
        if x == 0:
            xsend[k, 0, rows, :] = pltpu.roll(v, NP, 1)
        if x == NP - 1:
            xsend[k, 1, rows, :] = pltpu.roll(v, LANES - NP, 1)

    def halo_copies(k):
        return (
            (g > 0, rdma(xsend.at[k, 0], state.at[k, NP + 1], h_send.at[k, 0], h_recv.at[k, 0], gx=g - 1)),
            (g < sz.gx - 1, rdma(xsend.at[k, 1], state.at[k, 0], h_send.at[k, 1], h_recv.at[k, 1], gx=g + 1)),
            (y < sz.gy - 1, rdma(packs.at[k, 0], halos.at[k, 0], h_send.at[k, 2], h_recv.at[k, 2], gy=y + 1)),
            (y > 0, rdma(packs.at[k, 1], halos.at[k, 1], h_send.at[k, 3], h_recv.at[k, 3], gy=y - 1)),
        )

    def send_halos(k):
        for on, copy in halo_copies(k):
            @pl.when(on)
            def _():
                copy.start()

    def recv_halos(k):
        for on, ref, i in (
            (g < sz.gx - 1, state.at[k, NP + 1], 0),
            (g > 0, state.at[k, 0], 1),
            (y > 0, halos.at[k, 0], 2),
            (y < sz.gy - 1, halos.at[k, 1], 3),
        ):
            @pl.when(on)
            def _():
                wait(ref, h_recv.at[k, i])

    def drain_halos(k):
        for on, copy in halo_copies(k):
            @pl.when(on)
            def _():
                copy.wait_send()

    coef_copies = (
        (g < sz.gx - 1, rdma(asend, ca.at[0], r_send.at[0], r_send.at[2], gx=g + 1)),
        (y < sz.gy - 1, rdma(bpack, bhalo, r_send.at[1], r_send.at[3], gy=y + 1)),
    )
    runs = t != last_t

    @pl.when(runs)
    def _():
        for x in range(NP):
            for i in range(3):
                load(i, x).wait()
            for r, n in chunks:
                rows = pl.ds(r, n)
                s = sb[rows, :]
                a = clean(pltpu.roll(cx[x, rows, :], x, 1) + s, r, n)
                b = clean(pltpu.roll(cy[x, rows, :], x, 1) + s, r, n)
                ca[x + 1, rows, :] = a
                cb[x, rows, :] = b
                cc[x, rows, :] = 1.0 - 2.0 * s - a - b
                pltpu.store(bpack.at[rows, :], b, mask=at_lane(x - 1, n))
                if x == NP - 1:
                    asend[rows, :] = pltpu.roll(a, LANES - NP, 1)
                keep(0, x, r, n, clean(pltpu.roll(inc[x, rows, :], x, 1), r, n))

    @pl.when(t == last_t)
    def _():
        for x in range(NP):
            for i in range(3):
                load(i, x).wait()

    pl.semaphore_wait(barrier, len(group_a) + len(group_b) + has_out.astype(jnp.int32) + across.astype(jnp.int32))

    @pl.when(runs)
    def _():
        send_halos(0)
        for on, copy in coef_copies:
            @pl.when(on)
            def _():
                copy.start()

    def d_copy(x):
        to = t - 1
        if x >= half:
            to = jnp.where(t == XS, last_t, to)
        return rdma(dual.at[x, valid, :], later.at[x, valid, :], d_send.at[x], d_recv.at[x], tm=to)

    def d_pass(x):
        return rdma(later.at[x, valid, :], later.at[x, valid, :], d_send.at[NP + x], d_recv.at[x], tm=XS - 1)

    for x in range(NP):
        load(3, x).wait()

        @pl.when(t > 0)
        def _():
            d_copy(x).start()

    @pl.when(t == last_t)
    def _():
        for x in range(half, NP):
            wait(later.at[x, valid, :], d_recv.at[x])
            d_pass(x).start()

    def mixed(which, pair, emit):
        out = jnp.dot(wcat[which], tb[pair], preferred_element_type=F32)
        for j in range(2):
            for r, n in chunks:
                emit(2 * pair + j, r, n, out[r : r + n, j * LANES : (j + 1) * LANES])

    def put(pair, j, r, n, v):
        high = v.astype(BF16)
        low = (v - high.astype(F32)).astype(BF16)
        cols = pl.ds(j * LANES, LANES)
        tail = R - LANES
        main = min(n, LANES - r)
        if main > 0:
            tb[pair, pl.ds(r, main), cols] = high[:main]
            tb[pair, pl.ds(LANES + r, main), cols] = low[:main]
            tb[pair, pl.ds(2 * LANES + r, main), cols] = high[:main]
        if main < n:
            m = max(main, 0)
            o = 3 * LANES + r + m - LANES
            tb[pair, pl.ds(o, n - m), cols] = high[m:]
            tb[pair, pl.ds(o + tail, n - m), cols] = low[m:]
            tb[pair, pl.ds(o + 2 * tail, n - m), cols] = high[m:]

    def tangent(k, x, r, n):
        rows = pl.ds(r, n)
        v = state[k, x + 1, rows, :]
        edge = bhalo[rows, :] * halos[k, 0, rows, :]
        from_low = ca[x, rows, :] * state[k, x, rows, :] + jnp.where(at_lane(x - 1, n), edge, cb[x, rows, :] * v)
        from_high = state[k, x + 2, rows, :] + jnp.where(at_lane(x, n), halos[k, 1, rows, :], v)
        return cc[x, rows, :] * v + pltpu.roll(from_low, 1, 1) + sb[rows, :] * pltpu.roll(from_high, LANES - 1, 1)

    def adjoint(k, x, r, n):
        rows = pl.ds(r, n)
        w = state[k, x + 1, rows, :]
        low = state[k, x, rows, :] + jnp.where(at_lane(x - 1, n), halos[k, 0, rows, :], w)
        up_x = pltpu.roll(state[k, x + 2, rows, :], LANES - 1, 1)
        up_y = pltpu.roll(jnp.where(at_lane(x, n), halos[k, 1, rows, :], w), LANES - 1, 1)
        out = cc[x, rows, :] * w + ca[x + 1, rows, :] * up_x + cb[x, rows, :] * up_y
        return out + sb[rows, :] * pltpu.roll(low, 1, 1)

    def e_copy(x):
        to = t + 1
        if x >= half:
            to = jnp.where(t == XS - 1, 0, to)
        return rdma(end.at[x, valid, :], earlier.at[x, valid, :], e_send.at[x], e_recv.at[x], tm=to)

    def e_pass(x):
        return rdma(earlier.at[x, valid, :], earlier.at[x, valid, :], e_send.at[NP + x], e_recv.at[x], tm=XS)

    def keep_end(x, r, n, v):
        end[x, pl.ds(r, n), :] = pltpu.roll(v, (LANES - x) % LANES, 1)

    @pl.when(runs)
    def _():
        for k in range(STEPS):
            recv_halos(k)
            if k == 0:
                @pl.when(g > 0)
                def _():
                    wait(ca.at[0], r_send.at[2])

                @pl.when(y > 0)
                def _():
                    wait(bhalo, r_send.at[3])
            for pair in range(half):
                for j in range(2):
                    for r, n in chunks:
                        put(pair, j, r, n, tangent(k, 2 * pair + j, r, n))
                mixed(0, pair, functools.partial(keep, k + 1) if k < STEPS - 1 else keep_end)
                if k == STEPS - 1 and pair > 0:
                    e_copy(2 * pair - 2).start()
                    e_copy(2 * pair - 1).start()
            if k < STEPS - 1:
                send_halos(k + 1)
        e_copy(NP - 2).start()
        e_copy(NP - 1).start()

    @pl.when(t == 0)
    def _():
        for x in range(half, NP):
            wait(earlier.at[x, valid, :], e_recv.at[x])
            e_pass(x).start()

    for i in range(4, 8):
        for x in range(NP):
            load(i, x).wait()
    for x in range(NP):
        for r, n in chunks:
            rows = pl.ds(r, n)
            forc[x, rows, :] = forc[x, rows, :] - ev[x, rows, :] * dual[x, rows, :] - inc[x, rows, :]
            grad[x, rows, :] = grad[x, rows, :] - ob[x, rows, :] * inc[x, rows, :] - dual[x, rows, :]

    @pl.when(runs)
    def _():
        for k in range(STEPS, 2 * STEPS):
            for pair in range(half):
                for j in range(2):
                    x = 2 * pair + j
                    if k == STEPS:
                        wait(later.at[x, valid, :], d_recv.at[x])
                    for r, n in chunks:
                        if k == STEPS:
                            v = clean(pltpu.roll(later[x, pl.ds(r, n), :], x, 1), r, n)
                        else:
                            v = adjoint(k - 1, x, r, n)
                        put(pair, j, r, n, v)
                mixed(1, pair, functools.partial(keep, k))
            send_halos(k)
            recv_halos(k)
        for x in range(NP):
            for r, n in chunks:
                rows = pl.ds(r, n)
                back = adjoint(2 * STEPS - 1, x, r, n)
                grad[x, rows, :] = grad[x, rows, :] + pltpu.roll(back, (LANES - x) % LANES, 1)

    def squares(ref, x, total):
        for r, n in chunks:
            v = clean(ref[x, pl.ds(r, n), :], r, n)
            total = total + jnp.sum((v * v).reshape(n // 8, 8, LANES), axis=0)
        return total

    total = jnp.zeros((8, LANES), F32)
    for x in range(NP):
        total = squares(grad, x, total)

    @pl.when(t > 0)
    def _():
        for x in range(NP):
            wait(earlier.at[x, valid, :], e_recv.at[x])
            for r, n in chunks:
                rows = pl.ds(r, n)
                forc[x, rows, :] = forc[x, rows, :] + earlier[x, rows, :]

    for x in range(NP):
        total = squares(forc, x, total)

    stage_a[0] = total
    for i, p in enumerate(group_a):
        rdma(stage_a.at[0], stage_a.at[i + 1], p_send.at[0], p_recv.at[0], **peer_a(*p)).start()
    everyone = stage_a.at[pl.ds(1, len(group_a))]
    wait(everyone, p_recv.at[0])
    stage_b[0] = jnp.sum(stage_a[...], axis=0)
    for i, p in enumerate(group_b):
        rdma(stage_b.at[0], stage_b.at[i + 1], p_send.at[1], p_recv.at[1], **peer_b(*p)).start()
    everyone_b = stage_b.at[pl.ds(1, len(group_b))]
    wait(everyone_b, p_recv.at[1])
    global_sum = jnp.sum(jnp.sum(stage_b[...], axis=0), keepdims=True)
    count = 2 * L * NP * LANES * sz.tm * sz.gx * sz.gy
    root_mean = jnp.sqrt(global_sum / count + 1e-06)
    scale = jnp.minimum(1.0, 0.5 / root_mean)

    outs = []
    for x in range(NP):
        for r, n in chunks:
            rows = pl.ds(r, n)
            forc[x, rows, :] = dual[x, rows, :] + scale * forc[x, rows, :]
            grad[x, rows, :] = inc[x, rows, :] + scale * grad[x, rows, :]
        for i, (ref, out) in enumerate(((forc, out_dual), (grad, out_incr))):
            copy = pltpu.make_async_copy(ref.at[x, valid, :], out.at[0, :, x, :], store_sem.at[i, x])
            copy.start()
            outs.append(copy)

    wait(everyone, p_send.at[0])
    wait(everyone_b, p_send.at[1])

    @pl.when(runs)
    def _():
        for k in range(2 * STEPS):
            drain_halos(k)
        for on, copy in coef_copies:
            @pl.when(on)
            def _():
                copy.wait_send()
        for x in range(NP):
            e_copy(x).wait_send()

    @pl.when(t > 0)
    def _():
        for x in range(NP):
            d_copy(x).wait_send()

    @pl.when(t == last_t)
    def _():
        for x in range(half, NP):
            d_pass(x).wait_send()

    @pl.when(t == 0)
    def _():
        for x in range(half, NP):
            e_pass(x).wait_send()

    for copy in outs:
        copy.wait()


def solution(mesh):
    def local(increment, dual_state, forcing, gradient, courant_x, courant_y, error_var, obs_weight, diffusion, level_mix):
        _, levels, planes, lanes = increment.shape
        assert lanes == LANES
        sz = Sizes(mesh, levels, planes)
        R = sz.rows
        field = pltpu.VMEM((planes, R, LANES), F32)
        plane = pltpu.VMEM((R, LANES), F32)
        n = 2 * STEPS
        dma = pltpu.SemaphoreType.DMA
        any_spec = pl.BlockSpec(memory_space=pltpu.HBM)
        vmem_spec = pl.BlockSpec(memory_space=pltpu.VMEM)
        block = jax.ShapeDtypeStruct(increment.shape, F32)
        return pl.pallas_call(
            functools.partial(kernel, sz),
            name="saddle",
            out_shape=[block, block],
            in_specs=[any_spec] * 8 + [vmem_spec] * 2,
            out_specs=[any_spec] * 2,
            scratch_shapes=[field] * 11
            + [
                pltpu.VMEM((planes + 1, R, LANES), F32),
                field,
                field,
                plane,
                pltpu.VMEM((n, planes + 2, R, LANES), F32),
                pltpu.VMEM((n, 2, R, LANES), F32),
                pltpu.VMEM((n, 2, R, LANES), F32),
                pltpu.VMEM((n, 2, R, LANES), F32),
                plane,
                plane,
                plane,
                pltpu.VMEM((2, R, sz.depth), BF16),
                pltpu.VMEM((planes // 2, sz.depth, 2 * LANES), BF16),
                pltpu.VMEM((sz.xs * sz.gy * 2, 8, LANES), F32),
                pltpu.VMEM((sz.gx, 8, LANES), F32),
                dma((8, planes)),
                dma((2, planes)),
                dma((2 * planes,)),
                dma((planes,)),
                dma((2 * planes,)),
                dma((planes,)),
                dma((n, 4)),
                dma((n, 4)),
                dma((4,)),
                dma((2,)),
                dma((2,)),
            ],
            compiler_params=pltpu.CompilerParams(
                collective_id=0, has_side_effects=True, vmem_limit_bytes=60 * 1024 * 1024
            ),
        )(
            increment, dual_state, forcing, gradient, courant_x, courant_y, error_var, obs_weight,
            diffusion.reshape(1, -1), level_mix,
        )

    spec = P("tm", None, "gx", "gy")
    return jax.shard_map(
        local,
        mesh=mesh,
        in_specs=(spec,) * 8 + (P(), P()),
        out_specs=(spec, spec),
        check_vma=False,
    )
```

```python
import functools

import jax
import jax.numpy as jnp
from jax import lax
from jax.experimental import pallas as pl
from jax.experimental.pallas import tpu as pltpu
from jax.sharding import PartitionSpec as P

STEPS = 3
F32 = jnp.float32
BF16 = jnp.bfloat16
LANES = 128
MESH = pl.DeviceIdType.MESH


class Sizes:
    def __init__(self, mesh, levels, planes):
        self.tm, self.gx, self.gy = (mesh.shape[a] for a in ("tm", "gx", "gy"))
        self.xs = self.tm // 2
        self.levels = levels
        self.planes = planes
        self.rows = -(-levels // 16) * 16
        self.depth = 3 * self.rows


def kernel(
    sz,
    inc_h, dual_h, forc_h, grad_h, cx_h, cy_h, ev_h, ob_h, diff_h, mix_h,
    forc, grad, dual, inc, sums,
    cx, cy, ev, ob,
    later, earlier, end, side, acc,
    ca, cb, cc, sb, state, slim_out, slim_in, edges, xsend, bslim_out, bslim_in, bhalo, asend,
    diff_r, mix_r, wcat, tb, stage_a, stage_b,
    load_sem, d_send, d_recv, s_recv, e_send, e_recv, h_send, h_recv, c_send, c_recv, p_send, p_recv,
):
    NP, R, L = sz.planes, sz.rows, sz.levels
    XS = sz.xs
    t, g, y = (lax.axis_index(a) for a in ("tm", "gx", "gy"))
    xc, zh = lax.rem(t, XS), lax.div(t, XS)
    core, zl = lax.rem(g, 2), lax.div(g, 2)
    last_t = sz.tm - 1
    zchips = sz.gx // 2
    half = NP // 2
    scope = jax.named_scope

    def rdma(src, dst, ssem, rsem, **where):
        return pltpu.make_async_remote_copy(
            src_ref=src, dst_ref=dst, send_sem=ssem, recv_sem=rsem, device_id=where, device_id_type=MESH
        )

    def wait(ref, sem):
        pltpu.make_async_copy(ref, ref, sem).wait()

    barrier = pltpu.get_barrier_semaphore()
    group_a = [(dx, dy, dc) for dx in range(XS) for dy in range(sz.gy) for dc in range(2)][1:]
    group_b = [(dh, dl) for dh in range(2) for dl in range(zchips)][1:]

    def peer_a(dx, dy, dc):
        return {
            "tm": zh * XS + lax.rem(xc + dx, XS),
            "gy": lax.rem(y + dy, sz.gy),
            "gx": zl * 2 + lax.rem(core + dc, 2),
        }

    def peer_b(dh, dl):
        return {"tm": lax.rem(zh + dh, 2) * XS + xc, "gx": lax.rem(zl + dl, zchips) * 2 + core}

    def greet(where):
        pl.semaphore_signal(barrier, inc=1, device_id=where, device_id_type=MESH)

    for p in group_b:
        greet(peer_b(*p))
    for p in group_a:
        greet(peer_a(*p))
    outward = jnp.where(core == 0, g - 1, g + 1)
    has_out = (outward >= 0) & (outward < sz.gx)

    @pl.when(has_out)
    def _():
        greet({"gx": outward})

    across = jnp.where(t == XS - 1, 2, jnp.where((t == XS) | (t == XS + 1), 1, 0))

    @pl.when(t == XS - 1)
    def _():
        greet({"tm": XS})
        greet({"tm": XS + 1})

    @pl.when((t == XS) | (t == XS + 1))
    def _():
        greet({"tm": XS - 1})

    hbm = (inc_h, cx_h, cy_h, dual_h, forc_h, ev_h, ob_h, grad_h)
    local = (inc, cx, cy, dual, forc, ev, ob, grad)
    valid = pl.ds(0, L)

    def load(i):
        for x in range(NP):
            pltpu.make_async_copy(hbm[i].at[0, :, x, :], local[i].at[x, valid, :], load_sem.at[i]).start()

    def loaded(i):
        wait(local[i].at[:, valid, :], load_sem.at[i])

    diff_copy = pltpu.make_async_copy(diff_h, diff_r, load_sem.at[8])
    mix_copy = pltpu.make_async_copy(mix_h, mix_r, load_sem.at[9])
    diff_copy.start()
    for i in range(4):
        load(i)
    mix_copy.start()

    lane = lax.broadcasted_iota(jnp.int32, (8, LANES), 1)

    def at_lane(k, n):
        return jnp.broadcast_to((lane == k % LANES)[None], (n // 8, 8, LANES)).reshape(n, LANES)

    chunks = [(r, min(48, R - r)) for r in range(0, R, 48)]

    diff_copy.wait()
    lifted = jnp.concatenate([diff_r[...], jnp.zeros((1, 2 * LANES - L), F32)], axis=1)
    turned = jnp.broadcast_to(lifted, (LANES, 2 * LANES)).T
    sb[...] = turned[:R]

    def widen(m):
        high = m.astype(BF16).astype(F32)
        low = m - high
        tail = jnp.where(lane[:1] < R - LANES, high[:, LANES:], 0.0)
        tail_low = jnp.where(lane[:1] < R - LANES, low[:, LANES:], 0.0)
        k = R - LANES
        tails = tail + pltpu.roll(tail, k, 1) + pltpu.roll(tail_low, 2 * k, 1)
        whole = jnp.concatenate([high[:, :LANES], high[:, :LANES], low[:, :LANES], tails], axis=1)
        return whole[:, : sz.depth].astype(BF16)

    row = lax.broadcasted_iota(jnp.int32, (R, LANES), 0)

    def clean(v, r, n):
        return v if r + n <= L else jnp.where(row[r : r + n] < L, v, 0.0)

    @pl.when(g == 0)
    def _():
        for k in range(2 * STEPS):
            state[k, 0] = jnp.zeros((R, LANES), F32)
        ca[0] = jnp.zeros((R, LANES), F32)

    @pl.when(g == sz.gx - 1)
    def _():
        for k in range(2 * STEPS):
            state[k, NP + 1] = jnp.zeros((R, LANES), F32)

    @pl.when(y == 0)
    def _():
        for k in range(2 * STEPS):
            slim_in[k, 0] = jnp.zeros(slim_in.shape[2:], F32)
        bslim_in[...] = jnp.zeros(bslim_in.shape, F32)

    @pl.when(y == sz.gy - 1)
    def _():
        for k in range(2 * STEPS):
            slim_in[k, 1] = jnp.zeros(slim_in.shape[2:], F32)

    share = LANES // NP

    def slim(planes, dst, sides):
        for o in range(0, R // 8, share):
            acc = {}
            for j in range(min(share, R // 8 - o)):
                rows = pl.ds(8 * (o + j), 8)
                part = {}
                for x in range(NP):
                    v = planes(x, rows)
                    for side in sides:
                        part[side] = jnp.where(lane == (x + side - 1) % LANES, v, part[side]) if x else v
                for side in sides:
                    if j:
                        turned = pltpu.roll(part[side], NP * j, 1)
                        inside = (lane >= NP * j + side - 1) & (lane < NP * (j + 1) + side - 1)
                        acc[side] = jnp.where(inside, turned, acc[side])
                    else:
                        acc[side] = part[side]
            for side in sides:
                dst(side)[pl.ds(8 * (o // share), 8), :] = acc[side]

    def unslim(src, i):
        tile = src[pl.ds(8 * (i // share), 8), :]
        j = i % share
        return pltpu.roll(tile, LANES - NP * j, 1) if j else tile

    def keep(k, x, r, n, v):
        rows = pl.ds(r, n)
        state[k, x + 1, rows, :] = v
        if x == 0:
            xsend[k, 0, rows, :] = pltpu.roll(v, NP, 1)
        if x == NP - 1:
            xsend[k, 1, rows, :] = pltpu.roll(v, LANES - NP, 1)

    def halo_copies(k):
        return (
            (g > 0, xsend.at[k, 0], state.at[k, NP + 1], h_send.at[k, 0], h_recv.at[k, 0], {"gx": g - 1}),
            (g < sz.gx - 1, xsend.at[k, 1], state.at[k, 0], h_send.at[k, 1], h_recv.at[k, 1], {"gx": g + 1}),
            (y < sz.gy - 1, slim_out.at[k, 0], slim_in.at[k, 0], h_send.at[k, 2], h_recv.at[k, 2], {"gy": y + 1}),
            (y > 0, slim_out.at[k, 1], slim_in.at[k, 1], h_send.at[k, 3], h_recv.at[k, 3], {"gy": y - 1}),
        )

    def each(copies, act):
        for on, src, dst, ssem, rsem, where in copies:
            @pl.when(on)
            def _():
                act(rdma(src, dst, ssem, rsem, **where))

    def send_x(k):
        each(halo_copies(k)[:2], lambda c: c.start())

    def send_y(k):
        slim(lambda x, rows: state[k, x + 1, rows, :], lambda side: slim_out.at[k, side], (0, 1))
        each(halo_copies(k)[2:], lambda c: c.start())

    def recv_x(k):
        for on, ref, i in ((g < sz.gx - 1, state.at[k, NP + 1], 0), (g > 0, state.at[k, 0], 1)):
            @pl.when(on)
            def _():
                wait(ref, h_recv.at[k, i])

    def recv_y(k):
        for on, ref, i in ((y > 0, slim_in.at[k, 0], 2), (y < sz.gy - 1, slim_in.at[k, 1], 3)):
            @pl.when(on)
            def _():
                wait(ref, h_recv.at[k, i])
        for i in range(R // 8):
            rows = pl.ds(8 * i, 8)
            low = unslim(slim_in.at[k, 0], i)
            edges[0, rows, :] = bhalo[rows, :] * low if k < STEPS else low
            edges[1, rows, :] = unslim(slim_in.at[k, 1], i)

    coef_copies = (
        (g < sz.gx - 1, asend, ca.at[0], c_send.at[0], c_recv.at[0], {"gx": g + 1}),
        (y < sz.gy - 1, bslim_out, bslim_in, c_send.at[1], c_recv.at[1], {"gy": y + 1}),
    )
    runs = t != last_t
    for i in range(3):
        loaded(i)

    @pl.when(runs)
    def _():
        for x in range(NP):
            for r, n in chunks:
                rows = pl.ds(r, n)
                s = sb[rows, :]
                a = clean(pltpu.roll(cx[x, rows, :], x, 1) + s, r, n)
                b = clean(pltpu.roll(cy[x, rows, :], x, 1) + s, r, n)
                ca[x + 1, rows, :] = a
                cb[x, rows, :] = b
                cc[x, rows, :] = 1.0 - 2.0 * s - a - b
                if x == NP - 1:
                    asend[rows, :] = pltpu.roll(a, LANES - NP, 1)
                keep(0, x, r, n, clean(pltpu.roll(inc[x, rows, :], x, 1), r, n))
        slim(lambda x, rows: cb[x, rows, :], lambda side: bslim_out, (0,))

    loaded(3)
    with scope("wait_barrier"):
        pl.semaphore_wait(barrier, len(group_a) + len(group_b) + has_out.astype(jnp.int32) + across)

    @pl.when(runs)
    def _():
        send_x(0)
        send_y(0)
        each(coef_copies, lambda c: c.start())

    late = half - 1
    d_order = [0, late] + list(range(1, late))
    third = half // 4 + 1
    d_round, d_side, d_straight = d_order[:third], d_order[third : half - third], d_order[half - third :]
    e_order = list(range(1, late)) + [0, late]
    e_round = e_order[: 2 * third : 2]

    def pair_of(ref, p):
        return ref.at[pl.ds(2 * p, 2), valid, :]

    def d_copy(p):
        to = jnp.where(t == XS, last_t, t - 1) if p in d_round else t - 1
        return rdma(pair_of(dual, p), pair_of(later, p), d_send.at[0], d_recv.at[p], tm=to)

    def d_pass(p):
        return rdma(pair_of(later, p), pair_of(later, p), d_send.at[1], d_recv.at[p], tm=XS - 1)

    def s_copy(i):
        return rdma(pair_of(dual, d_side[i]), pair_of(side, i), d_send.at[0], s_recv.at[i], tm=XS + 1)

    def s_pass(i):
        p = d_side[i]
        return rdma(pair_of(side, i), pair_of(later, p), d_send.at[1], d_recv.at[p], tm=XS - 1)

    @pl.when(t > 0)
    def _():
        for p in d_round:
            d_copy(p).start()

    @pl.when(t == XS)
    def _():
        for i in range(len(d_side)):
            s_copy(i).start()

    @pl.when((t > 0) & (t != XS))
    def _():
        for p in d_side + d_straight:
            d_copy(p).start()

    for i in range(4, 8):
        load(i)

    @pl.when(t == last_t)
    def _():
        for p in d_round:
            with scope(f"relay_d{p}"):
                wait(pair_of(later, p), d_recv.at[p])
            d_pass(p).start()

    mix_copy.wait()
    mix = jnp.concatenate([mix_r[...], jnp.zeros((L, 2 * LANES - L), F32)], axis=1)
    mix = jnp.concatenate([mix, jnp.zeros((2 * LANES - L, 2 * LANES), F32)], axis=0)
    wcat[0] = widen(mix[:R])
    wcat[1] = widen(mix.T[:R])

    def mixed(which, pair, emit):
        out = jnp.dot(wcat[which], tb[pair], preferred_element_type=F32)
        for j in range(2):
            for r, n in chunks:
                emit(2 * pair + j, r, n, out[r : r + n, j * LANES : (j + 1) * LANES])

    def put(pair, j, r, n, v):
        high = v.astype(BF16)
        low = (v - high.astype(F32)).astype(BF16)
        cols = pl.ds(j * LANES, LANES)
        tail = R - LANES
        main = min(n, LANES - r)
        if main > 0:
            tb[pair, pl.ds(r, main), cols] = high[:main]
            tb[pair, pl.ds(LANES + r, main), cols] = low[:main]
            tb[pair, pl.ds(2 * LANES + r, main), cols] = high[:main]
        if main < n:
            m = max(main, 0)
            o = 3 * LANES + r + m - LANES
            tb[pair, pl.ds(o, n - m), cols] = high[m:]
            tb[pair, pl.ds(o + tail, n - m), cols] = low[m:]
            tb[pair, pl.ds(o + 2 * tail, n - m), cols] = high[m:]

    def tangent(k, x, r, n):
        rows = pl.ds(r, n)
        v = state[k, x + 1, rows, :]
        from_low = ca[x, rows, :] * state[k, x, rows, :] + jnp.where(
            at_lane(x - 1, n), edges[0, rows, :], cb[x, rows, :] * v
        )
        from_high = state[k, x + 2, rows, :] + jnp.where(at_lane(x, n), edges[1, rows, :], v)
        return cc[x, rows, :] * v + pltpu.roll(from_low, 1, 1) + sb[rows, :] * pltpu.roll(from_high, LANES - 1, 1)

    def adjoint(k, x, r, n):
        rows = pl.ds(r, n)
        w = state[k, x + 1, rows, :]
        low = state[k, x, rows, :] + jnp.where(at_lane(x - 1, n), edges[0, rows, :], w)
        up_x = pltpu.roll(state[k, x + 2, rows, :], LANES - 1, 1)
        up_y = pltpu.roll(jnp.where(at_lane(x, n), edges[1, rows, :], w), LANES - 1, 1)
        out = cc[x, rows, :] * w + ca[x + 1, rows, :] * up_x + cb[x, rows, :] * up_y
        return out + sb[rows, :] * pltpu.roll(low, 1, 1)

    def e_copy(p):
        to = jnp.where(t == XS - 1, 0, t + 1) if p in e_round else t + 1
        return rdma(pair_of(end, p), pair_of(earlier, p), e_send.at[0], e_recv.at[p], tm=to)

    def e_pass(p):
        return rdma(pair_of(earlier, p), pair_of(earlier, p), e_send.at[1], e_recv.at[p], tm=XS)

    def keep_end(x, r, n, v):
        end[x, pl.ds(r, n), :] = pltpu.roll(v, (LANES - x) % LANES, 1)

    @pl.when(runs)
    def _():
        for k in range(STEPS):
            with scope(f"halo_y{k}"):
                if k == 0:
                    @pl.when(y > 0)
                    def _():
                        wait(bslim_in, c_recv.at[1])
                    for i in range(R // 8):
                        bhalo[pl.ds(8 * i, 8), :] = unslim(bslim_in, i)
                recv_y(k)
            for i, pair in enumerate(e_order):
                if pair == 0:
                    with scope(f"halo_x{k}"):
                        recv_x(k)
                        if k == 0:
                            @pl.when(g > 0)
                            def _():
                                wait(ca.at[0], c_recv.at[0])
                for j in range(2):
                    for r, n in chunks:
                        put(pair, j, r, n, tangent(k, 2 * pair + j, r, n))
                mixed(0, pair, functools.partial(keep, k + 1) if k < STEPS - 1 else keep_end)
                if k == STEPS - 1 and i > 0:
                    e_copy(e_order[i - 1]).start()
            if k < STEPS - 1:
                send_x(k + 1)
                send_y(k + 1)
            else:
                e_copy(e_order[-1]).start()
            if k == STEPS - 2:
                @pl.when(t == XS)
                def _():
                    for p in d_straight:
                        d_copy(p).start()

                @pl.when(t == XS + 1)
                def _():
                    for i in range(len(d_side)):
                        with scope(f"side{i}"):
                            wait(pair_of(side, i), s_recv.at[i])
                        s_pass(i).start()

    for i in range(4, 8):
        loaded(i)
    for x in range(NP):
        for r, n in chunks:
            rows = pl.ds(r, n)
            forc[x, rows, :] = forc[x, rows, :] - ev[x, rows, :] * dual[x, rows, :] - inc[x, rows, :]
            grad[x, rows, :] = grad[x, rows, :] - ob[x, rows, :] * inc[x, rows, :] - dual[x, rows, :]

    @pl.when(runs)
    def _():
        for k in range(STEPS, 2 * STEPS):
            if k > STEPS:
                with scope(f"halo_y{k}"):
                    recv_y(k - 1)
            for i, pair in enumerate(d_order if k == STEPS else e_order):
                if k == STEPS:
                    if i % 2 == 0 and i // 2 < len(e_round):
                        @pl.when(t == 0)
                        def _():
                            p = e_round[i // 2]
                            with scope(f"relay_e{p}"):
                                wait(pair_of(earlier, p), e_recv.at[p])
                            e_pass(p).start()
                    with scope(f"wait_d{pair}"):
                        wait(pair_of(later, pair), d_recv.at[pair])
                elif pair == 0:
                    with scope(f"halo_x{k}"):
                        recv_x(k - 1)
                for j in range(2):
                    x = 2 * pair + j
                    for r, n in chunks:
                        if k == STEPS:
                            v = clean(pltpu.roll(later[x, pl.ds(r, n), :], x, 1), r, n)
                        else:
                            v = adjoint(k - 1, x, r, n)
                        put(pair, j, r, n, v)
                mixed(1, pair, functools.partial(keep, k))
                if k == STEPS and i == 1:
                    send_x(k)
            if k > STEPS:
                send_x(k)
            send_y(k)

    def squared(v, r, n):
        v = clean(v, r, n)
        return jnp.sum((v * v).reshape(n // 8, 8, LANES), axis=0)

    def add_earlier():
        total = acc[...]
        for p in e_order:
            with scope(f"wait_e{p}"):
                wait(pair_of(earlier, p), e_recv.at[p])
            for x in (2 * p, 2 * p + 1):
                for r, n in chunks:
                    rows = pl.ds(r, n)
                    v = forc[x, rows, :] + earlier[x, rows, :]
                    forc[x, rows, :] = v
                    total = total + squared(v, r, n)
        acc[...] = total

    acc[...] = jnp.zeros((8, LANES), F32)

    @pl.when((t > 0) & (t != XS))
    def _():
        add_earlier()

    @pl.when(runs)
    def _():
        k = 2 * STEPS - 1
        with scope("halo_last"):
            recv_y(k)
            recv_x(k)
        total = acc[...]
        for x in range(NP):
            for r, n in chunks:
                rows = pl.ds(r, n)
                back = adjoint(k, x, r, n)
                v = grad[x, rows, :] + pltpu.roll(back, (LANES - x) % LANES, 1)
                grad[x, rows, :] = v
                total = total + squared(v, r, n)
        acc[...] = total

    @pl.when(t == XS)
    def _():
        add_earlier()

    for on, ref in ((t == 0, forc), (t == last_t, grad)):
        @pl.when(on)
        def _():
            total = acc[...]
            for x in range(NP):
                for r, n in chunks:
                    total = total + squared(ref[x, pl.ds(r, n), :], r, n)
            acc[...] = total

    stage_a[0] = jnp.sum(acc[...], axis=0, keepdims=True)
    for i, p in enumerate(group_a):
        rdma(stage_a.at[0], stage_a.at[i + 1], p_send.at[0], p_recv.at[0], **peer_a(*p)).start()
    everyone = stage_a.at[pl.ds(1, len(group_a))]
    with scope("sum_a"):
        wait(everyone, p_recv.at[0])
    stage_b[0] = jnp.sum(stage_a[...], axis=0)
    for i, p in enumerate(group_b):
        rdma(stage_b.at[0], stage_b.at[i + 1], p_send.at[1], p_recv.at[1], **peer_b(*p)).start()
    everyone_b = stage_b.at[pl.ds(1, len(group_b))]

    wait(everyone, p_send.at[0])

    @pl.when(runs)
    def _():
        for k in range(2 * STEPS):
            each(halo_copies(k), lambda c: c.wait_send())
        each(coef_copies, lambda c: c.wait_send())
        wait(end.at[:, valid, :], e_send.at[0])

    @pl.when(t > 0)
    def _():
        wait(dual.at[:, valid, :], d_send.at[0])

    @pl.when(t == last_t)
    def _():
        wait(later.at[pl.ds(0, 2 * len(d_round)), valid, :], d_send.at[1])

    @pl.when(t == XS + 1)
    def _():
        wait(side.at[pl.ds(0, 2 * len(d_side)), valid, :], d_send.at[1])

    @pl.when(t == 0)
    def _():
        wait(later.at[pl.ds(0, 2 * len(e_round)), valid, :], e_send.at[1])

    with scope("sum_b"):
        wait(everyone_b, p_recv.at[1])
    sums[...] = jnp.sum(stage_b[...], axis=0)
    wait(everyone_b, p_send.at[1])


def finish(sz, forc, grad, dual, inc, sums, out_dual, out_incr, done, sem):
    chunks = [(r, min(48, sz.rows - r)) for r in range(0, sz.rows, 48)]
    valid = pl.ds(0, sz.levels)
    global_sum = jnp.sum(sums[...], keepdims=True)
    count = 2 * sz.levels * sz.planes * LANES * sz.tm * sz.gx * sz.gy
    root_mean = jnp.sqrt(global_sum / count + 1e-06)
    scale = jnp.minimum(1.0, 0.5 / root_mean)
    outs = (out_dual, out_incr)
    for x in range(sz.planes):
        for i, (base, step) in enumerate(((dual, forc), (inc, grad))):
            for r, n in chunks:
                rows = pl.ds(r, n)
                done[i, x, rows, :] = base[x, rows, :] + scale * step[x, rows, :]
            pltpu.make_async_copy(done.at[i, x, valid, :], outs[i].at[0, :, x, :], sem.at[i]).start()
    for i in range(2):
        whole = done.at[i, :, valid, :]
        pltpu.make_async_copy(whole, whole, sem.at[i]).wait()


def solution(mesh):
    def local(increment, dual_state, forcing, gradient, courant_x, courant_y, error_var, obs_weight, diffusion, level_mix):
        _, levels, planes, lanes = increment.shape
        assert lanes == LANES
        sz = Sizes(mesh, levels, planes)
        R = sz.rows
        field = pltpu.VMEM((planes, R, LANES), F32)
        plane = pltpu.VMEM((R, LANES), F32)
        n = 2 * STEPS
        thin = 8 * -(-R * planes // (8 * LANES))
        slim = pltpu.VMEM((thin, LANES), F32)
        dma = pltpu.SemaphoreType.DMA
        any_spec = pl.BlockSpec(memory_space=pltpu.HBM)
        vmem_spec = pl.BlockSpec(memory_space=pltpu.VMEM)
        block = jax.ShapeDtypeStruct(increment.shape, F32)
        kept = pl.pallas_call(
            functools.partial(kernel, sz),
            name="saddle",
            out_shape=[pltpu.VMEM((planes, R, LANES), F32)] * 4 + [pltpu.VMEM((1, LANES), F32)],
            in_specs=[any_spec] * 10,
            out_specs=[pl.BlockSpec(memory_space=pltpu.VMEM)] * 5,
            scratch_shapes=[field] * 7
            + [
                pltpu.VMEM((planes // 2, R, LANES), F32),
                pltpu.VMEM((8, LANES), F32),
                pltpu.VMEM((planes + 1, R, LANES), F32),
                field,
                field,
                plane,
                pltpu.VMEM((n, planes + 2, R, LANES), F32),
                pltpu.VMEM((n, 2, thin, LANES), F32),
                pltpu.VMEM((n, 2, thin, LANES), F32),
                pltpu.VMEM((2, R, LANES), F32),
                pltpu.VMEM((n, 2, R, LANES), F32),
                slim,
                slim,
                plane,
                plane,
                pltpu.VMEM((1, levels), F32),
                pltpu.VMEM((levels, levels), F32),
                pltpu.VMEM((2, R, sz.depth), BF16),
                pltpu.VMEM((planes // 2, sz.depth, 2 * LANES), BF16),
                pltpu.VMEM((sz.xs * sz.gy * 2, 1, LANES), F32),
                pltpu.VMEM((sz.gx, 1, LANES), F32),
                dma((10,)),
                dma((2,)),
                dma((planes // 2,)),
                dma((planes // 2,)),
                dma((2,)),
                dma((planes // 2,)),
                dma((n, 4)),
                dma((n, 4)),
                dma((2,)),
                dma((2,)),
                dma((2,)),
                dma((2,)),
            ],
            compiler_params=pltpu.CompilerParams(
                collective_id=0, has_side_effects=True, vmem_limit_bytes=60_000_000
            ),
        )(
            increment, dual_state, forcing, gradient, courant_x, courant_y, error_var, obs_weight,
            diffusion.reshape(1, -1), level_mix,
        )
        return pl.pallas_call(
            functools.partial(finish, sz),
            name="finish",
            out_shape=[block, block],
            in_specs=[vmem_spec] * 5,
            out_specs=[any_spec] * 2,
            scratch_shapes=[pltpu.VMEM((2, planes, R, LANES), F32), dma((2,))],
            compiler_params=pltpu.CompilerParams(vmem_limit_bytes=6_000_000),
        )(*kept)

    spec = P("tm", None, "gx", "gy")
    return jax.shard_map(
        local,
        mesh=mesh,
        in_specs=(spec,) * 8 + (P(), P()),
        out_specs=(spec, spec),
        check_vma=False,
    )
```

```python
import functools

import jax
import jax.numpy as jnp
from jax import lax
from jax.experimental import pallas as pl
from jax.experimental.pallas import tpu as pltpu
from jax.sharding import PartitionSpec as P

STEPS = 3
F32 = jnp.float32
BF16 = jnp.bfloat16
LANES = 128
MESH = pl.DeviceIdType.MESH


class Sizes:
    def __init__(self, mesh, levels, planes):
        self.tm, self.gx, self.gy = (mesh.shape[a] for a in ("tm", "gx", "gy"))
        self.xs = self.tm // 2
        self.levels = levels
        self.planes = planes
        self.rows = -(-levels // 16) * 16
        self.depth = 3 * self.rows


def kernel(
    sz,
    inc_h, dual_h, forc_h, grad_h, cx_h, cy_h, ev_h, ob_h, diff_h, mix_h,
    forc, grad, dual, inc, sums,
    cx, cy, ev, ob,
    later, earlier, end, side, acc,
    ca, cb, cc, sb, state, slim_out, slim_in, edges, xsend, bslim_out, bslim_in, bhalo, asend,
    diff_r, mix_r, wcat, tb, stage_a, stage_b,
    load_sem, d_send, d_recv, s_recv, e_send, e_recv, h_send, h_recv, c_send, c_recv, p_send, p_recv,
):
    NP, R, L = sz.planes, sz.rows, sz.levels
    XS = sz.xs
    t, g, y = (lax.axis_index(a) for a in ("tm", "gx", "gy"))
    xc, zh = lax.rem(t, XS), lax.div(t, XS)
    core, zl = lax.rem(g, 2), lax.div(g, 2)
    last_t = sz.tm - 1
    zchips = sz.gx // 2
    half = NP // 2
    helper = XS + 2
    scope = jax.named_scope

    def rdma(src, dst, ssem, rsem, **where):
        return pltpu.make_async_remote_copy(
            src_ref=src, dst_ref=dst, send_sem=ssem, recv_sem=rsem, device_id=where, device_id_type=MESH
        )

    def wait(ref, sem):
        pltpu.make_async_copy(ref, ref, sem).wait()

    barrier = pltpu.get_barrier_semaphore()
    group_a = [(dx, dy, dc) for dx in range(XS) for dy in range(sz.gy) for dc in range(2)][1:]
    group_b = [(dh, dl) for dh in range(2) for dl in range(zchips)][1:]

    def peer_a(dx, dy, dc):
        return {
            "tm": zh * XS + lax.rem(xc + dx, XS),
            "gy": lax.rem(y + dy, sz.gy),
            "gx": zl * 2 + lax.rem(core + dc, 2),
        }

    def peer_b(dh, dl):
        return {"tm": lax.rem(zh + dh, 2) * XS + xc, "gx": lax.rem(zl + dl, zchips) * 2 + core}

    def greet(where):
        pl.semaphore_signal(barrier, inc=1, device_id=where, device_id_type=MESH)

    for p in group_b:
        greet(peer_b(*p))
    for p in group_a:
        greet(peer_a(*p))
    outward = jnp.where(core == 0, g - 1, g + 1)
    has_out = (outward >= 0) & (outward < sz.gx)

    @pl.when(has_out)
    def _():
        greet({"gx": outward})

    other = zl * 2 + 1 - core
    across = jnp.where((t == XS - 1) | (t == XS), 2, jnp.where((t == 0) | (t == helper), 1, 0))

    @pl.when((t == 0) | (t == XS))
    def _():
        greet({"tm": XS - t, "gx": other})

    @pl.when(t == XS - 1)
    def _():
        greet({"tm": XS})
        greet({"tm": helper})

    @pl.when((t == XS) | (t == helper))
    def _():
        greet({"tm": XS - 1})

    hbm = (inc_h, cx_h, cy_h, dual_h, forc_h, ev_h, ob_h, grad_h)
    local = (inc, cx, cy, dual, forc, ev, ob, grad)
    valid = pl.ds(0, L)

    def load(i):
        for x in range(NP):
            pltpu.make_async_copy(hbm[i].at[0, :, x, :], local[i].at[x, valid, :], load_sem.at[i]).start()

    def loaded(i):
        wait(local[i].at[:, valid, :], load_sem.at[i])

    diff_copy = pltpu.make_async_copy(diff_h, diff_r, load_sem.at[8])
    mix_copy = pltpu.make_async_copy(mix_h, mix_r, load_sem.at[9])
    diff_copy.start()
    for i in range(4):
        load(i)
    mix_copy.start()

    lane = lax.broadcasted_iota(jnp.int32, (8, LANES), 1)

    def at_lane(k, n):
        return jnp.broadcast_to((lane == k % LANES)[None], (n // 8, 8, LANES)).reshape(n, LANES)

    chunks = [(r, min(48, R - r)) for r in range(0, R, 48)]

    diff_copy.wait()
    lifted = jnp.concatenate([diff_r[...], jnp.zeros((1, 2 * LANES - L), F32)], axis=1)
    turned = jnp.broadcast_to(lifted, (LANES, 2 * LANES)).T
    sb[...] = turned[:R]

    def widen(m):
        high = m.astype(BF16).astype(F32)
        low = m - high
        tail = jnp.where(lane[:1] < R - LANES, high[:, LANES:], 0.0)
        tail_low = jnp.where(lane[:1] < R - LANES, low[:, LANES:], 0.0)
        k = R - LANES
        tails = tail + pltpu.roll(tail, k, 1) + pltpu.roll(tail_low, 2 * k, 1)
        whole = jnp.concatenate([high[:, :LANES], high[:, :LANES], low[:, :LANES], tails], axis=1)
        return whole[:, : sz.depth].astype(BF16)

    row = lax.broadcasted_iota(jnp.int32, (R, LANES), 0)

    def clean(v, r, n):
        return v if r + n <= L else jnp.where(row[r : r + n] < L, v, 0.0)

    @pl.when(g == 0)
    def _():
        for k in range(2 * STEPS):
            state[k, 0] = jnp.zeros((R, LANES), F32)
        ca[0] = jnp.zeros((R, LANES), F32)

    @pl.when(g == sz.gx - 1)
    def _():
        for k in range(2 * STEPS):
            state[k, NP + 1] = jnp.zeros((R, LANES), F32)

    @pl.when(y == 0)
    def _():
        for k in range(2 * STEPS):
            slim_in[k, 0] = jnp.zeros(slim_in.shape[2:], F32)
        bslim_in[...] = jnp.zeros(bslim_in.shape, F32)

    @pl.when(y == sz.gy - 1)
    def _():
        for k in range(2 * STEPS):
            slim_in[k, 1] = jnp.zeros(slim_in.shape[2:], F32)

    share = LANES // NP

    def slim(planes, dst, sides):
        for o in range(0, R // 8, share):
            acc = {}
            for j in range(min(share, R // 8 - o)):
                rows = pl.ds(8 * (o + j), 8)
                part = {}
                for x in range(NP):
                    v = planes(x, rows)
                    for side in sides:
                        part[side] = jnp.where(lane == (x + side - 1) % LANES, v, part[side]) if x else v
                for side in sides:
                    if j:
                        turned = pltpu.roll(part[side], NP * j, 1)
                        inside = (lane >= NP * j + side - 1) & (lane < NP * (j + 1) + side - 1)
                        acc[side] = jnp.where(inside, turned, acc[side])
                    else:
                        acc[side] = part[side]
            for side in sides:
                dst(side)[pl.ds(8 * (o // share), 8), :] = acc[side]

    def unslim(src, i):
        tile = src[pl.ds(8 * (i // share), 8), :]
        j = i % share
        return pltpu.roll(tile, LANES - NP * j, 1) if j else tile

    def keep(k, x, r, n, v):
        rows = pl.ds(r, n)
        state[k, x + 1, rows, :] = v
        if x == 0:
            xsend[k, 0, rows, :] = pltpu.roll(v, NP, 1)
        if x == NP - 1:
            xsend[k, 1, rows, :] = pltpu.roll(v, LANES - NP, 1)

    def halo_copies(k):
        return (
            (g > 0, xsend.at[k, 0], state.at[k, NP + 1], h_send.at[k, 0], h_recv.at[k, 0], {"gx": g - 1}),
            (g < sz.gx - 1, xsend.at[k, 1], state.at[k, 0], h_send.at[k, 1], h_recv.at[k, 1], {"gx": g + 1}),
            (y < sz.gy - 1, slim_out.at[k, 0], slim_in.at[k, 0], h_send.at[k, 2], h_recv.at[k, 2], {"gy": y + 1}),
            (y > 0, slim_out.at[k, 1], slim_in.at[k, 1], h_send.at[k, 3], h_recv.at[k, 3], {"gy": y - 1}),
        )

    def each(copies, act):
        for on, src, dst, ssem, rsem, where in copies:
            @pl.when(on)
            def _():
                act(rdma(src, dst, ssem, rsem, **where))

    def send_x(k):
        each(halo_copies(k)[:2], lambda c: c.start())

    def send_y(k):
        slim(lambda x, rows: state[k, x + 1, rows, :], lambda side: slim_out.at[k, side], (0, 1))
        each(halo_copies(k)[2:], lambda c: c.start())

    def recv_x(k):
        for on, ref, i in ((g < sz.gx - 1, state.at[k, NP + 1], 0), (g > 0, state.at[k, 0], 1)):
            @pl.when(on)
            def _():
                wait(ref, h_recv.at[k, i])

    def recv_y(k):
        for on, ref, i in ((y > 0, slim_in.at[k, 0], 2), (y < sz.gy - 1, slim_in.at[k, 1], 3)):
            @pl.when(on)
            def _():
                wait(ref, h_recv.at[k, i])
        for i in range(R // 8):
            rows = pl.ds(8 * i, 8)
            low = unslim(slim_in.at[k, 0], i)
            edges[0, rows, :] = bhalo[rows, :] * low if k < STEPS else low
            edges[1, rows, :] = unslim(slim_in.at[k, 1], i)

    coef_copies = (
        (g < sz.gx - 1, asend, ca.at[0], c_send.at[0], c_recv.at[0], {"gx": g + 1}),
        (y < sz.gy - 1, bslim_out, bslim_in, c_send.at[1], c_recv.at[1], {"gy": y + 1}),
    )
    runs = t != last_t
    for i in range(3):
        loaded(i)

    @pl.when(runs)
    def _():
        for x in range(NP):
            for r, n in chunks:
                rows = pl.ds(r, n)
                s = sb[rows, :]
                a = clean(pltpu.roll(cx[x, rows, :], x, 1) + s, r, n)
                b = clean(pltpu.roll(cy[x, rows, :], x, 1) + s, r, n)
                ca[x + 1, rows, :] = a
                cb[x, rows, :] = b
                cc[x, rows, :] = 1.0 - 2.0 * s - a - b
                if x == NP - 1:
                    asend[rows, :] = pltpu.roll(a, LANES - NP, 1)
                keep(0, x, r, n, clean(pltpu.roll(inc[x, rows, :], x, 1), r, n))
        slim(lambda x, rows: cb[x, rows, :], lambda side: bslim_out, (0,))

    loaded(3)
    with scope("wait_barrier"):
        pl.semaphore_wait(barrier, len(group_a) + len(group_b) + has_out.astype(jnp.int32) + across)

    @pl.when(runs)
    def _():
        send_x(0)
        send_y(0)
        each(coef_copies, lambda c: c.start())

    late = half - 1
    d_order = [0, late] + list(range(1, late))
    third = half // 4 + 1
    d_round, d_side, d_straight = d_order[:third], d_order[third : 2 * third], d_order[2 * third :]
    e_order = list(range(1, late)) + [0, late]
    straight = core == lax.rem(zl, 2)
    around = (t == XS - 1) & jnp.logical_not(straight)

    def pair_of(ref, p):
        return ref.at[pl.ds(2 * p, 2), valid, :]

    def d_copy(p):
        to = jnp.where(t == XS, last_t, t - 1) if p in d_round else t - 1
        return rdma(pair_of(dual, p), pair_of(later, p), d_send.at[0], d_recv.at[p], tm=to)

    def d_pass(p):
        return rdma(pair_of(later, p), pair_of(later, p), d_send.at[1], d_recv.at[p], tm=XS - 1)

    def s_copy(i):
        return rdma(pair_of(dual, d_side[i]), pair_of(side, i), d_send.at[0], s_recv.at[i], tm=helper)

    def s_pass(i):
        p = d_side[i]
        return rdma(pair_of(side, i), pair_of(later, p), d_send.at[1], d_recv.at[p], tm=XS - 1)

    @pl.when(t > 0)
    def _():
        for p in d_round:
            d_copy(p).start()

    @pl.when(t == XS)
    def _():
        for i in range(len(d_side)):
            s_copy(i).start()

    @pl.when((t > 0) & (t != XS))
    def _():
        for p in d_side + d_straight:
            d_copy(p).start()

    for i in range(4, 8):
        load(i)

    @pl.when(t == last_t)
    def _():
        for p in d_round:
            with scope(f"relay_d{p}"):
                wait(pair_of(later, p), d_recv.at[p])
            d_pass(p).start()

    mix_copy.wait()
    mix = jnp.concatenate([mix_r[...], jnp.zeros((L, 2 * LANES - L), F32)], axis=1)
    mix = jnp.concatenate([mix, jnp.zeros((2 * LANES - L, 2 * LANES), F32)], axis=0)
    wcat[0] = widen(mix[:R])
    wcat[1] = widen(mix.T[:R])

    def mixed(which, pair, emit):
        out = jnp.dot(wcat[which], tb[pair], preferred_element_type=F32)
        for j in range(2):
            for r, n in chunks:
                emit(2 * pair + j, r, n, out[r : r + n, j * LANES : (j + 1) * LANES])

    def put(pair, j, r, n, v):
        high = v.astype(BF16)
        low = (v - high.astype(F32)).astype(BF16)
        cols = pl.ds(j * LANES, LANES)
        tail = R - LANES
        main = min(n, LANES - r)
        if main > 0:
            tb[pair, pl.ds(r, main), cols] = high[:main]
            tb[pair, pl.ds(LANES + r, main), cols] = low[:main]
            tb[pair, pl.ds(2 * LANES + r, main), cols] = high[:main]
        if main < n:
            m = max(main, 0)
            o = 3 * LANES + r + m - LANES
            tb[pair, pl.ds(o, n - m), cols] = high[m:]
            tb[pair, pl.ds(o + tail, n - m), cols] = low[m:]
            tb[pair, pl.ds(o + 2 * tail, n - m), cols] = high[m:]

    def tangent(k, x, r, n):
        rows = pl.ds(r, n)
        v = state[k, x + 1, rows, :]
        from_low = ca[x, rows, :] * state[k, x, rows, :] + jnp.where(
            at_lane(x - 1, n), edges[0, rows, :], cb[x, rows, :] * v
        )
        from_high = state[k, x + 2, rows, :] + jnp.where(at_lane(x, n), edges[1, rows, :], v)
        return cc[x, rows, :] * v + pltpu.roll(from_low, 1, 1) + sb[rows, :] * pltpu.roll(from_high, LANES - 1, 1)

    def adjoint(k, x, r, n):
        rows = pl.ds(r, n)
        w = state[k, x + 1, rows, :]
        low = state[k, x, rows, :] + jnp.where(at_lane(x - 1, n), edges[0, rows, :], w)
        up_x = pltpu.roll(state[k, x + 2, rows, :], LANES - 1, 1)
        up_y = pltpu.roll(jnp.where(at_lane(x, n), edges[1, rows, :], w), LANES - 1, 1)
        out = cc[x, rows, :] * w + ca[x + 1, rows, :] * up_x + cb[x, rows, :] * up_y
        return out + sb[rows, :] * pltpu.roll(low, 1, 1)

    def e_copy(p):
        to, column = jnp.where(around, 0, t + 1), jnp.where(around, other, g)
        return rdma(pair_of(end, p), pair_of(earlier, p), e_send.at[0], e_recv.at[p], tm=to, gx=column)

    def e_pass(p):
        return rdma(pair_of(earlier, p), pair_of(earlier, p), e_send.at[1], e_recv.at[p], tm=XS, gx=other)

    def keep_end(x, r, n, v):
        end[x, pl.ds(r, n), :] = pltpu.roll(v, (LANES - x) % LANES, 1)

    @pl.when(runs)
    def _():
        for k in range(STEPS):
            with scope(f"halo_y{k}"):
                if k == 0:
                    @pl.when(y > 0)
                    def _():
                        wait(bslim_in, c_recv.at[1])
                    for i in range(R // 8):
                        bhalo[pl.ds(8 * i, 8), :] = unslim(bslim_in, i)
                recv_y(k)
            for i, pair in enumerate(e_order):
                if pair == 0:
                    with scope(f"halo_x{k}"):
                        recv_x(k)
                        if k == 0:
                            @pl.when(g > 0)
                            def _():
                                wait(ca.at[0], c_recv.at[0])
                for j in range(2):
                    for r, n in chunks:
                        put(pair, j, r, n, tangent(k, 2 * pair + j, r, n))
                mixed(0, pair, functools.partial(keep, k + 1) if k < STEPS - 1 else keep_end)
                if k == STEPS - 1 and i == 2:
                    for p in e_order[:i]:
                        e_copy(p).start()
            if k < STEPS - 1:
                send_x(k + 1)
                send_y(k + 1)
            else:
                for p in e_order[2:]:
                    e_copy(p).start()
            if k == STEPS - 2:
                @pl.when(t == XS)
                def _():
                    for p in d_straight:
                        d_copy(p).start()

                @pl.when(t == helper)
                def _():
                    for i in range(len(d_side)):
                        with scope(f"side{i}"):
                            wait(pair_of(side, i), s_recv.at[i])
                        s_pass(i).start()

    for i in range(4, 8):
        loaded(i)
    for x in range(NP):
        for r, n in chunks:
            rows = pl.ds(r, n)
            forc[x, rows, :] = forc[x, rows, :] - ev[x, rows, :] * dual[x, rows, :] - inc[x, rows, :]
            grad[x, rows, :] = grad[x, rows, :] - ob[x, rows, :] * inc[x, rows, :] - dual[x, rows, :]

    @pl.when(runs)
    def _():
        for k in range(STEPS, 2 * STEPS):
            if k > STEPS:
                with scope(f"halo_y{k}"):
                    recv_y(k - 1)
            for i, pair in enumerate(d_order if k == STEPS else e_order):
                if k == STEPS:
                    @pl.when((t == 0) & straight)
                    def _():
                        p = e_order[i]
                        with scope(f"relay_e{p}"):
                            wait(pair_of(earlier, p), e_recv.at[p])
                        e_pass(p).start()
                    with scope(f"wait_d{pair}"):
                        wait(pair_of(later, pair), d_recv.at[pair])
                elif pair == 0:
                    with scope(f"halo_x{k}"):
                        recv_x(k - 1)
                for j in range(2):
                    x = 2 * pair + j
                    for r, n in chunks:
                        if k == STEPS:
                            v = clean(pltpu.roll(later[x, pl.ds(r, n), :], x, 1), r, n)
                        else:
                            v = adjoint(k - 1, x, r, n)
                        put(pair, j, r, n, v)
                mixed(1, pair, functools.partial(keep, k))
                if k == STEPS and i == 1:
                    send_x(k)
            if k > STEPS:
                send_x(k)
            send_y(k)

    def squared(v, r, n):
        v = clean(v, r, n)
        return jnp.sum((v * v).reshape(n // 8, 8, LANES), axis=0)

    def add_earlier():
        total = acc[...]
        for p in e_order:
            with scope(f"wait_e{p}"):
                wait(pair_of(earlier, p), e_recv.at[p])
            for x in (2 * p, 2 * p + 1):
                for r, n in chunks:
                    rows = pl.ds(r, n)
                    v = forc[x, rows, :] + earlier[x, rows, :]
                    forc[x, rows, :] = v
                    total = total + squared(v, r, n)
        acc[...] = total

    acc[...] = jnp.zeros((8, LANES), F32)

    @pl.when((t > 0) & (t != XS))
    def _():
        add_earlier()

    @pl.when(runs)
    def _():
        k = 2 * STEPS - 1
        with scope("halo_last"):
            recv_y(k)
            recv_x(k)
        total = acc[...]
        for x in range(NP):
            for r, n in chunks:
                rows = pl.ds(r, n)
                back = adjoint(k, x, r, n)
                v = grad[x, rows, :] + pltpu.roll(back, (LANES - x) % LANES, 1)
                grad[x, rows, :] = v
                total = total + squared(v, r, n)
        acc[...] = total

    @pl.when(t == XS)
    def _():
        add_earlier()

    for on, ref in ((t == 0, forc), (t == last_t, grad)):
        @pl.when(on)
        def _():
            total = acc[...]
            for x in range(NP):
                for r, n in chunks:
                    total = total + squared(ref[x, pl.ds(r, n), :], r, n)
            acc[...] = total

    stage_a[0] = jnp.sum(acc[...], axis=0, keepdims=True)
    for i, p in enumerate(group_a):
        rdma(stage_a.at[0], stage_a.at[i + 1], p_send.at[0], p_recv.at[0], **peer_a(*p)).start()
    everyone = stage_a.at[pl.ds(1, len(group_a))]
    with scope("sum_a"):
        wait(everyone, p_recv.at[0])
    stage_b[0] = jnp.sum(stage_a[...], axis=0)
    for i, p in enumerate(group_b):
        rdma(stage_b.at[0], stage_b.at[i + 1], p_send.at[1], p_recv.at[1], **peer_b(*p)).start()
    everyone_b = stage_b.at[pl.ds(1, len(group_b))]

    wait(everyone, p_send.at[0])

    @pl.when(runs)
    def _():
        for k in range(2 * STEPS):
            each(halo_copies(k), lambda c: c.wait_send())
        each(coef_copies, lambda c: c.wait_send())
        wait(end.at[:, valid, :], e_send.at[0])

    @pl.when(t > 0)
    def _():
        wait(dual.at[:, valid, :], d_send.at[0])

    @pl.when(t == last_t)
    def _():
        wait(later.at[pl.ds(0, 2 * len(d_round)), valid, :], d_send.at[1])

    @pl.when(t == helper)
    def _():
        wait(side.at[pl.ds(0, 2 * len(d_side)), valid, :], d_send.at[1])

    @pl.when((t == 0) & straight)
    def _():
        wait(earlier.at[:, valid, :], e_send.at[1])

    with scope("sum_b"):
        wait(everyone_b, p_recv.at[1])
    sums[...] = jnp.sum(stage_b[...], axis=0)
    wait(everyone_b, p_send.at[1])


def finish(sz, forc, grad, dual, inc, sums, out_dual, out_incr, done, sem):
    chunks = [(r, min(48, sz.rows - r)) for r in range(0, sz.rows, 48)]
    valid = pl.ds(0, sz.levels)
    global_sum = jnp.sum(sums[...], keepdims=True)
    count = 2 * sz.levels * sz.planes * LANES * sz.tm * sz.gx * sz.gy
    root_mean = jnp.sqrt(global_sum / count + 1e-06)
    scale = jnp.minimum(1.0, 0.5 / root_mean)
    outs = (out_dual, out_incr)
    for x in range(sz.planes):
        for i, (base, step) in enumerate(((dual, forc), (inc, grad))):
            for r, n in chunks:
                rows = pl.ds(r, n)
                done[i, x, rows, :] = base[x, rows, :] + scale * step[x, rows, :]
            pltpu.make_async_copy(done.at[i, x, valid, :], outs[i].at[0, :, x, :], sem.at[i]).start()
    for i in range(2):
        whole = done.at[i, :, valid, :]
        pltpu.make_async_copy(whole, whole, sem.at[i]).wait()


def solution(mesh):
    def local(increment, dual_state, forcing, gradient, courant_x, courant_y, error_var, obs_weight, diffusion, level_mix):
        _, levels, planes, lanes = increment.shape
        assert lanes == LANES
        sz = Sizes(mesh, levels, planes)
        R = sz.rows
        field = pltpu.VMEM((planes, R, LANES), F32)
        plane = pltpu.VMEM((R, LANES), F32)
        n = 2 * STEPS
        thin = 8 * -(-R * planes // (8 * LANES))
        slim = pltpu.VMEM((thin, LANES), F32)
        dma = pltpu.SemaphoreType.DMA
        any_spec = pl.BlockSpec(memory_space=pltpu.HBM)
        vmem_spec = pl.BlockSpec(memory_space=pltpu.VMEM)
        block = jax.ShapeDtypeStruct(increment.shape, F32)
        kept = pl.pallas_call(
            functools.partial(kernel, sz),
            name="saddle",
            out_shape=[pltpu.VMEM((planes, R, LANES), F32)] * 4 + [pltpu.VMEM((1, LANES), F32)],
            in_specs=[any_spec] * 10,
            out_specs=[pl.BlockSpec(memory_space=pltpu.VMEM)] * 5,
            scratch_shapes=[field] * 7
            + [
                pltpu.VMEM((planes // 2, R, LANES), F32),
                pltpu.VMEM((8, LANES), F32),
                pltpu.VMEM((planes + 1, R, LANES), F32),
                field,
                field,
                plane,
                pltpu.VMEM((n, planes + 2, R, LANES), F32),
                pltpu.VMEM((n, 2, thin, LANES), F32),
                pltpu.VMEM((n, 2, thin, LANES), F32),
                pltpu.VMEM((2, R, LANES), F32),
                pltpu.VMEM((n, 2, R, LANES), F32),
                slim,
                slim,
                plane,
                plane,
                pltpu.VMEM((1, levels), F32),
                pltpu.VMEM((levels, levels), F32),
                pltpu.VMEM((2, R, sz.depth), BF16),
                pltpu.VMEM((planes // 2, sz.depth, 2 * LANES), BF16),
                pltpu.VMEM((sz.xs * sz.gy * 2, 1, LANES), F32),
                pltpu.VMEM((sz.gx, 1, LANES), F32),
                dma((10,)),
                dma((2,)),
                dma((planes // 2,)),
                dma((planes // 2,)),
                dma((2,)),
                dma((planes // 2,)),
                dma((n, 4)),
                dma((n, 4)),
                dma((2,)),
                dma((2,)),
                dma((2,)),
                dma((2,)),
            ],
            compiler_params=pltpu.CompilerParams(
                collective_id=0, has_side_effects=True, vmem_limit_bytes=60_000_000
            ),
        )(
            increment, dual_state, forcing, gradient, courant_x, courant_y, error_var, obs_weight,
            diffusion.reshape(1, -1), level_mix,
        )
        return pl.pallas_call(
            functools.partial(finish, sz),
            name="finish",
            out_shape=[block, block],
            in_specs=[vmem_spec] * 5,
            out_specs=[any_spec] * 2,
            scratch_shapes=[pltpu.VMEM((2, planes, R, LANES), F32), dma((2,))],
            compiler_params=pltpu.CompilerParams(vmem_limit_bytes=6_000_000),
        )(*kept)

    spec = P("tm", None, "gx", "gy")
    return jax.shard_map(
        local,
        mesh=mesh,
        in_specs=(spec,) * 8 + (P(), P()),
        out_specs=(spec, spec),
        check_vma=False,
    )
```

```python
import functools

import jax
import jax.numpy as jnp
from jax import lax
from jax.experimental import pallas as pl
from jax.experimental.pallas import tpu as pltpu
from jax.sharding import PartitionSpec as P

STEPS = 3
F32 = jnp.float32
BF16 = jnp.bfloat16
LANES = 128
MESH = pl.DeviceIdType.MESH


class Sizes:
    def __init__(self, mesh, levels, planes):
        self.tm, self.gx, self.gy = (mesh.shape[a] for a in ("tm", "gx", "gy"))
        self.xs = self.tm // 2
        self.levels = levels
        self.planes = planes
        self.rows = -(-levels // 16) * 16
        self.depth = 3 * self.rows


def kernel(
    sz,
    inc_h, dual_h, forc_h, grad_h, cx_h, cy_h, ev_h, ob_h, diff_h, mix_h,
    forc, grad, dual, inc, sums,
    cx, cy, ev, ob,
    later, earlier, end, side, acc, cols, zed, bown,
    ca, cb, cc, sb, state, slim_out, slim_in, edges, xsend, bslim_out, bslim_in, bhalo, asend,
    diff_r, mix_r, wcat, tb, stage_a, stage_b,
    load_sem, d_send, d_recv, s_recv, e_send, e_recv, h_send, h_recv, c_send, c_recv, p_send, p_recv,
):
    NP, R, L = sz.planes, sz.rows, sz.levels
    XS = sz.xs
    t, g, y = (lax.axis_index(a) for a in ("tm", "gx", "gy"))
    xc, zh = lax.rem(t, XS), lax.div(t, XS)
    core, zl = lax.rem(g, 2), lax.div(g, 2)
    last_t = sz.tm - 1
    zchips = sz.gx // 2
    half = NP // 2
    helper = XS + 2
    scope = jax.named_scope

    def rdma(src, dst, ssem, rsem, **where):
        return pltpu.make_async_remote_copy(
            src_ref=src, dst_ref=dst, send_sem=ssem, recv_sem=rsem, device_id=where, device_id_type=MESH
        )

    def wait(ref, sem):
        pltpu.make_async_copy(ref, ref, sem).wait()

    barrier = pltpu.get_barrier_semaphore()
    group_a = [(dx, dy, dc) for dx in range(XS) for dy in range(sz.gy) for dc in range(2)][1:]
    group_b = [(dh, dl) for dh in range(2) for dl in range(zchips)][1:]

    def peer_a(dx, dy, dc):
        return {
            "tm": zh * XS + lax.rem(xc + dx, XS),
            "gy": lax.rem(y + dy, sz.gy),
            "gx": zl * 2 + lax.rem(core + dc, 2),
        }

    def peer_b(dh, dl):
        return {"tm": lax.rem(zh + dh, 2) * XS + xc, "gx": lax.rem(zl + dl, zchips) * 2 + core}

    def greet(where):
        pl.semaphore_signal(barrier, inc=1, device_id=where, device_id_type=MESH)

    for p in group_b:
        greet(peer_b(*p))
    for p in group_a:
        greet(peer_a(*p))
    outward = jnp.where(core == 0, g - 1, g + 1)
    has_out = (outward >= 0) & (outward < sz.gx)

    @pl.when(has_out)
    def _():
        greet({"gx": outward})

    other = zl * 2 + 1 - core
    across = jnp.where((t == XS - 1) | (t == XS), 2, jnp.where((t == 0) | (t == helper), 1, 0))

    @pl.when((t == 0) | (t == XS))
    def _():
        greet({"tm": XS - t, "gx": other})

    @pl.when(t == XS - 1)
    def _():
        greet({"tm": XS})
        greet({"tm": helper})

    @pl.when((t == XS) | (t == helper))
    def _():
        greet({"tm": XS - 1})

    hbm = (inc_h, cx_h, cy_h, dual_h, forc_h, ev_h, ob_h, grad_h)
    local = (inc, cx, cy, dual, forc, ev, ob, grad)
    valid = pl.ds(0, L)

    def load(i):
        for x in range(NP):
            pltpu.make_async_copy(hbm[i].at[0, :, x, :], local[i].at[x, valid, :], load_sem.at[i]).start()

    def loaded(i):
        wait(local[i].at[:, valid, :], load_sem.at[i])

    diff_copy = pltpu.make_async_copy(diff_h, diff_r, load_sem.at[8])
    mix_copy = pltpu.make_async_copy(mix_h, mix_r, load_sem.at[9])
    diff_copy.start()
    for i in range(4):
        load(i)
    mix_copy.start()

    lane = lax.broadcasted_iota(jnp.int32, (8, LANES), 1)

    def at_lane(k, n):
        return jnp.broadcast_to((lane == k % LANES)[None], (n // 8, 8, LANES)).reshape(n, LANES)

    chunks = [(r, min(48, R - r)) for r in range(0, R, 48)]

    diff_copy.wait()
    lifted = jnp.concatenate([diff_r[...], jnp.zeros((1, 2 * LANES - L), F32)], axis=1)
    turned = jnp.broadcast_to(lifted, (LANES, 2 * LANES)).T
    sb[...] = turned[:R]

    def widen(m):
        high = m.astype(BF16).astype(F32)
        low = m - high
        tail = jnp.where(lane[:1] < R - LANES, high[:, LANES:], 0.0)
        tail_low = jnp.where(lane[:1] < R - LANES, low[:, LANES:], 0.0)
        k = R - LANES
        tails = tail + pltpu.roll(tail, k, 1) + pltpu.roll(tail_low, 2 * k, 1)
        whole = jnp.concatenate([high[:, :LANES], high[:, :LANES], low[:, :LANES], tails], axis=1)
        return whole[:, : sz.depth].astype(BF16)

    row = lax.broadcasted_iota(jnp.int32, (R, LANES), 0)

    def clean(v, r, n):
        return v if r + n <= L else jnp.where(row[r : r + n] < L, v, 0.0)

    @pl.when(g == 0)
    def _():
        for k in range(2 * STEPS):
            state[k, 0] = jnp.zeros((R, LANES), F32)
        ca[0] = jnp.zeros((R, LANES), F32)

    @pl.when(g == sz.gx - 1)
    def _():
        for k in range(2 * STEPS):
            state[k, NP + 1] = jnp.zeros((R, LANES), F32)

    @pl.when(y == 0)
    def _():
        for k in range(2 * STEPS):
            slim_in[k, 0] = jnp.zeros(slim_in.shape[2:], F32)
        bslim_in[...] = jnp.zeros(bslim_in.shape, F32)

    @pl.when(y == sz.gy - 1)
    def _():
        for k in range(2 * STEPS):
            slim_in[k, 1] = jnp.zeros(slim_in.shape[2:], F32)

    share = LANES // NP

    def slim_tiles(tile, dst, e):
        for o in range(0, R // 8, share):
            acc = tile(pl.ds(8 * o, 8))
            for j in range(1, min(share, R // 8 - o)):
                turned = pltpu.roll(tile(pl.ds(8 * (o + j), 8)), NP * j, 1)
                inside = (lane >= NP * j + e - 1) & (lane < NP * (j + 1) + e - 1)
                acc = jnp.where(inside, turned, acc)
            dst[pl.ds(8 * (o // share), 8), :] = acc

    def slim(planes, dst, sides):
        for e in sides:
            def tile(rows):
                part = planes(0, rows)
                for x in range(1, NP):
                    part = jnp.where(lane == x + e - 1, planes(x, rows), part)
                return part

            slim_tiles(tile, dst(e), e)

    def unslim(src, i):
        tile = src[pl.ds(8 * (i // share), 8), :]
        j = i % share
        return pltpu.roll(tile, LANES - NP * j, 1) if j else tile

    def keep(k, x, r, n, v):
        rows = pl.ds(r, n)
        state[k, x + 1, rows, :] = v
        if x == 0:
            xsend[k, 0, rows, :] = pltpu.roll(v, NP, 1)
        if x == NP - 1:
            xsend[k, 1, rows, :] = pltpu.roll(v, LANES - NP, 1)

    def halo_copies(k):
        return (
            (g > 0, xsend.at[k, 0], state.at[k, NP + 1], h_send.at[k, 0], h_recv.at[k, 0], {"gx": g - 1}),
            (g < sz.gx - 1, xsend.at[k, 1], state.at[k, 0], h_send.at[k, 1], h_recv.at[k, 1], {"gx": g + 1}),
            (y < sz.gy - 1, slim_out.at[k, 0], slim_in.at[k, 0], h_send.at[k, 2], h_recv.at[k, 2], {"gy": y + 1}),
            (y > 0, slim_out.at[k, 1], slim_in.at[k, 1], h_send.at[k, 3], h_recv.at[k, 3], {"gy": y - 1}),
        )

    def each(copies, act):
        for on, src, dst, ssem, rsem, where in copies:
            @pl.when(on)
            def _():
                act(rdma(src, dst, ssem, rsem, **where))

    def send_x(k):
        each(halo_copies(k)[:2], lambda c: c.start())

    def send_y(k):
        slim(lambda x, rows: state[k, x + 1, rows, :], lambda side: slim_out.at[k, side], (0, 1))
        each(halo_copies(k)[2:], lambda c: c.start())

    def recv_x(k):
        for on, ref, i in ((g < sz.gx - 1, state.at[k, NP + 1], 0), (g > 0, state.at[k, 0], 1)):
            @pl.when(on)
            def _():
                wait(ref, h_recv.at[k, i])

    def recv_y(k):
        for on, ref, i in ((y > 0, slim_in.at[k, 0], 2), (y < sz.gy - 1, slim_in.at[k, 1], 3)):
            @pl.when(on)
            def _():
                wait(ref, h_recv.at[k, i])
        for i in range(R // 8):
            rows = pl.ds(8 * i, 8)
            low = unslim(slim_in.at[k, 0], i)
            edges[0, rows, :] = bhalo[rows, :] * low if k < STEPS else low
            edges[1, rows, :] = unslim(slim_in.at[k, 1], i)

    coef_copies = (
        (g < sz.gx - 1, asend, ca.at[0], c_send.at[0], c_recv.at[0], {"gx": g + 1}),
        (y < sz.gy - 1, bslim_out, bslim_in, c_send.at[1], c_recv.at[1], {"gy": y + 1}),
    )
    runs = t != last_t
    def turned_field(ref, x, r, n):
        return pltpu.roll(ref[x, pl.ds(r, n), :], x, 1)

    loaded(0)

    @pl.when(runs)
    def _():
        for x in range(NP):
            for r, n in chunks:
                keep(0, x, r, n, clean(turned_field(inc, x, r, n), r, n))
        slim(lambda x, rows: state[0, x + 1, rows, :], lambda side: slim_out.at[0, side], (0, 1))

    loaded(1)
    loaded(2)

    @pl.when(runs)
    def _():
        for x in range(NP):
            for r, n in chunks:
                rows = pl.ds(r, n)
                cb[x, rows, :] = clean(turned_field(cy, x, r, n) + sb[rows, :], r, n)
        slim(lambda x, rows: cb[x, rows, :], lambda side: bslim_out, (0,))
        for r, n in chunks:
            rows = pl.ds(r, n)
            a = clean(turned_field(cx, NP - 1, r, n) + sb[rows, :], r, n)
            asend[rows, :] = pltpu.roll(a, LANES - NP, 1)

    loaded(3)
    with scope("wait_barrier"):
        pl.semaphore_wait(barrier, len(group_a) + len(group_b) + has_out.astype(jnp.int32) + across)

    @pl.when(runs)
    def _():
        send_x(0)
        each(halo_copies(0)[2:], lambda c: c.start())
        each(coef_copies, lambda c: c.start())

    late = half - 1
    d_order = [0, late] + list(range(1, late))
    third = half // 4 + 1
    d_round, d_side, d_straight = d_order[:third], d_order[third : 2 * third], d_order[2 * third :]
    e_order = list(range(1, late)) + [0, late]
    straight = core == lax.rem(zl, 2)
    around = (t == XS - 1) & jnp.logical_not(straight)

    def pair_of(ref, p):
        return ref.at[pl.ds(2 * p, 2), valid, :]

    def d_copy(p):
        to = jnp.where(t == XS, last_t, t - 1) if p in d_round else t - 1
        return rdma(pair_of(dual, p), pair_of(later, p), d_send.at[0], d_recv.at[p], tm=to)

    def d_pass(p):
        return rdma(pair_of(later, p), pair_of(later, p), d_send.at[1], d_recv.at[p], tm=XS - 1)

    def s_copy(i):
        return rdma(pair_of(dual, d_side[i]), pair_of(side, i), d_send.at[0], s_recv.at[i], tm=helper)

    def s_pass(i):
        p = d_side[i]
        return rdma(pair_of(side, i), pair_of(later, p), d_send.at[1], d_recv.at[p], tm=XS - 1)

    @pl.when(t > 0)
    def _():
        for p in d_round:
            d_copy(p).start()

    @pl.when(t == XS)
    def _():
        for i in range(len(d_side)):
            s_copy(i).start()

    @pl.when((t > 0) & (t != XS))
    def _():
        for p in d_side + d_straight:
            d_copy(p).start()

    for i in range(4, 8):
        load(i)

    @pl.when(t == last_t)
    def _():
        for p in d_round:
            with scope(f"relay_d{p}"):
                wait(pair_of(later, p), d_recv.at[p])
            d_pass(p).start()

    @pl.when(runs)
    def _():
        for x in range(NP):
            for r, n in chunks:
                rows = pl.ds(r, n)
                s = sb[rows, :]
                a = clean(turned_field(cx, x, r, n) + s, r, n)
                ca[x + 1, rows, :] = a
                cc[x, rows, :] = 1.0 - 2.0 * s - a - cb[x, rows, :]

    mix_copy.wait()
    mix = jnp.concatenate([mix_r[...], jnp.zeros((L, 2 * LANES - L), F32)], axis=1)
    mix = jnp.concatenate([mix, jnp.zeros((2 * LANES - L, 2 * LANES), F32)], axis=0)
    wcat[0] = widen(mix[:R])
    wcat[1] = widen(mix.T[:R])

    def mixed(which, pair, emit):
        out = jnp.dot(wcat[which], tb[pair], preferred_element_type=F32)
        for j in range(2):
            for r, n in chunks:
                emit(2 * pair + j, r, n, out[r : r + n, j * LANES : (j + 1) * LANES])

    def put(pair, j, r, n, v):
        high = v.astype(BF16)
        low = (v - high.astype(F32)).astype(BF16)
        cols = pl.ds(j * LANES, LANES)
        tail = R - LANES
        main = min(n, LANES - r)
        if main > 0:
            tb[pair, pl.ds(r, main), cols] = high[:main]
            tb[pair, pl.ds(LANES + r, main), cols] = low[:main]
            tb[pair, pl.ds(2 * LANES + r, main), cols] = high[:main]
        if main < n:
            m = max(main, 0)
            o = 3 * LANES + r + m - LANES
            tb[pair, pl.ds(o, n - m), cols] = high[m:]
            tb[pair, pl.ds(o + tail, n - m), cols] = low[m:]
            tb[pair, pl.ds(o + 2 * tail, n - m), cols] = high[m:]

    def edge_of(side, rows, edge):
        return edges[side, rows, :] if edge else 0.0

    def tangent(k, x, r, n, edge=True):
        rows = pl.ds(r, n)
        v = state[k, x + 1, rows, :]
        from_low = ca[x, rows, :] * state[k, x, rows, :] + jnp.where(
            at_lane(x - 1, n), edge_of(0, rows, edge), cb[x, rows, :] * v
        )
        from_high = state[k, x + 2, rows, :] + jnp.where(at_lane(x, n), edge_of(1, rows, edge), v)
        return cc[x, rows, :] * v + pltpu.roll(from_low, 1, 1) + sb[rows, :] * pltpu.roll(from_high, LANES - 1, 1)

    def adjoint(k, x, r, n, edge=True):
        rows = pl.ds(r, n)
        w = state[k, x + 1, rows, :]
        low = state[k, x, rows, :] + jnp.where(at_lane(x - 1, n), edge_of(0, rows, edge), w)
        up_x = pltpu.roll(state[k, x + 2, rows, :], LANES - 1, 1)
        up_y = pltpu.roll(jnp.where(at_lane(x, n), edge_of(1, rows, edge), w), LANES - 1, 1)
        out = cc[x, rows, :] * w + ca[x + 1, rows, :] * up_x + cb[x, rows, :] * up_y
        return out + sb[rows, :] * pltpu.roll(low, 1, 1)

    def tangent_edges(rows):
        first = pltpu.roll(edges[0, rows, :], 1, 1)
        return first, sb[rows, :] * pltpu.roll(edges[1, rows, :], LANES - 1, 1)

    def adjoint_edges(rows):
        first = sb[rows, :] * pltpu.roll(edges[0, rows, :], 1, 1)
        return first, bown[rows, :] * pltpu.roll(edges[1, rows, :], LANES - 1, 1)

    inner_pairs, outer_pairs = list(range(1, half - 1)), [0, half - 1]
    inner = list(range(2, NP - 2))
    outer = [0, 1, NP - 2, NP - 1]

    def step_inner(k, which, stencil, emit):
        for pair in inner_pairs:
            for j in range(2):
                for r, n in chunks:
                    put(pair, j, r, n, stencil(k, 2 * pair + j, r, n, False))
            mixed(which, pair, emit)

    def step_edges(which, stencil_edges):
        for r, n in chunks:
            for j, v in enumerate(stencil_edges(pl.ds(r, n))):
                put(half, j, r, n, v)
        zed[...] = jnp.dot(wcat[which], tb[half], preferred_element_type=F32)

    def step_outer(k, which, stencil, emit):
        for pair in outer_pairs:
            for j in range(2):
                for r, n in chunks:
                    put(pair, j, r, n, stencil(k, 2 * pair + j, r, n))
            mixed(which, pair, emit)

    def advance(k, which, stencil, stencil_edges, extra_y, extra_x, after):
        emit = functools.partial(keep, k + 1)
        step_inner(k, which, stencil, emit)
        for i in range(R // 8):
            rows = pl.ds(8 * i, 8)
            part = [None, None]
            for x in inner:
                v = state[k + 1, x + 1, rows, :]
                for e in range(2):
                    part[e] = v if part[e] is None else jnp.where(lane == x + e - 1, v, part[e])
            for e in range(2):
                cols[e, rows, :] = part[e]
        with scope(f"halo_y{k}"):
            extra_y()
            recv_y(k)
        step_edges(which, stencil_edges)
        with scope(f"halo_x{k}"):
            extra_x()
            recv_x(k)
        step_outer(k, which, stencil, emit)
        send_x(k + 1)
        for i in range(R // 8):
            rows = pl.ds(8 * i, 8)
            for e in range(2):
                v = cols[e, rows, :] + zed[rows, pl.ds((1 - e) * LANES, LANES)]
                for x in outer:
                    v = jnp.where(lane == (x + e - 1) % LANES, state[k + 1, x + 1, rows, :], v)
                cols[e, rows, :] = v
        for e in range(2):
            slim_tiles(lambda rows: cols[e, rows, :], slim_out.at[k + 1, e], e)
        each(halo_copies(k + 1)[2:], lambda c: c.start())
        after()
        for x in inner:
            for e in range(2):
                pltpu.store(state.at[k + 1, x + 1], cols[e], mask=at_lane(x + e - 1, R))

    def e_copy(p):
        to, column = jnp.where(around, 0, t + 1), jnp.where(around, other, g)
        return rdma(pair_of(end, p), pair_of(earlier, p), e_send.at[0], e_recv.at[p], tm=to, gx=column)

    def e_pass(p):
        return rdma(pair_of(earlier, p), pair_of(earlier, p), e_send.at[1], e_recv.at[p], tm=XS, gx=other)

    def keep_end(x, r, n, v):
        end[x, pl.ds(r, n), :] = pltpu.roll(v, (LANES - x) % LANES, 1)

    def nothing():
        pass

    def first_y():
        @pl.when(y > 0)
        def _():
            wait(bslim_in, c_recv.at[1])
        for i in range(R // 8):
            bhalo[pl.ds(8 * i, 8), :] = unslim(bslim_in, i)

    def first_x():
        @pl.when(g > 0)
        def _():
            wait(ca.at[0], c_recv.at[0])

    def cross():
        @pl.when(t == XS)
        def _():
            for p in d_straight:
                d_copy(p).start()

        @pl.when(t == helper)
        def _():
            for i in range(len(d_side)):
                with scope(f"side{i}"):
                    wait(pair_of(side, i), s_recv.at[i])
                s_pass(i).start()

    def keep_turned(x, r, n, v):
        end[x, pl.ds(r, n), :] = v

    @pl.when(runs)
    def _():
        for k in range(STEPS - 1):
            advance(
                k, 0, tangent, tangent_edges,
                nothing if k else first_y, nothing if k else first_x, cross if k == STEPS - 2 else nothing,
            )
        k = STEPS - 1
        step_inner(k, 0, tangent, keep_turned)
        for i in range(R // 8):
            bown[pl.ds(8 * i, 8), :] = unslim(bslim_out, i)
        with scope(f"halo_y{k}"):
            recv_y(k)
        step_edges(0, tangent_edges)
        for i, pair in enumerate(inner_pairs):
            for x in (2 * pair, 2 * pair + 1):
                for r, n in chunks:
                    rows = pl.ds(r, n)
                    v = end[x, rows, :]
                    v = jnp.where(at_lane(x, n), v + zed[rows, pl.ds(0, LANES)], v)
                    v = jnp.where(at_lane(x - 1, n), v + zed[rows, pl.ds(LANES, LANES)], v)
                    keep_end(x, r, n, v)
            if i == 1:
                for p in e_order[:2]:
                    e_copy(p).start()
        with scope(f"halo_x{k}"):
            recv_x(k)
        step_outer(k, 0, tangent, keep_end)
        for p in e_order[2:]:
            e_copy(p).start()

    for i in range(4, 8):
        loaded(i)
    for x in range(NP):
        for r, n in chunks:
            rows = pl.ds(r, n)
            forc[x, rows, :] = forc[x, rows, :] - ev[x, rows, :] * dual[x, rows, :] - inc[x, rows, :]
            grad[x, rows, :] = grad[x, rows, :] - ob[x, rows, :] * inc[x, rows, :] - dual[x, rows, :]

    @pl.when(runs)
    def _():
        k = STEPS
        for i, pair in enumerate(d_order):
            @pl.when((t == 0) & straight)
            def _():
                p = e_order[i]
                with scope(f"relay_e{p}"):
                    wait(pair_of(earlier, p), e_recv.at[p])
                e_pass(p).start()

            with scope(f"wait_d{pair}"):
                wait(pair_of(later, pair), d_recv.at[pair])
            for j in range(2):
                x = 2 * pair + j
                for r, n in chunks:
                    put(pair, j, r, n, clean(turned_field(later, x, r, n), r, n))
            mixed(1, pair, functools.partial(keep, k))
            if i == 1:
                send_x(k)
        send_y(k)
        for k in range(STEPS, 2 * STEPS - 1):
            advance(k, 1, adjoint, adjoint_edges, nothing, nothing, nothing)
        for x in inner:
            for r, n in chunks:
                state[0, x + 1, pl.ds(r, n), :] = adjoint(2 * STEPS - 1, x, r, n, False)

    def squared(v, r, n):
        v = clean(v, r, n)
        return jnp.sum((v * v).reshape(n // 8, 8, LANES), axis=0)

    def add_earlier():
        total = acc[...]
        for p in e_order:
            with scope(f"wait_e{p}"):
                wait(pair_of(earlier, p), e_recv.at[p])
            for x in (2 * p, 2 * p + 1):
                for r, n in chunks:
                    rows = pl.ds(r, n)
                    v = forc[x, rows, :] + earlier[x, rows, :]
                    forc[x, rows, :] = v
                    total = total + squared(v, r, n)
        acc[...] = total

    acc[...] = jnp.zeros((8, LANES), F32)

    @pl.when((t > 0) & (t != XS - 1) & (t != XS))
    def _():
        add_earlier()

    @pl.when(runs)
    def _():
        k = 2 * STEPS - 1
        with scope("halo_last"):
            recv_y(k)
        total = acc[...]
        for r, n in chunks:
            rows = pl.ds(r, n)
            first, last = adjoint_edges(rows)
            zed[rows, pl.ds(0, LANES)] = first
            zed[rows, pl.ds(LANES, LANES)] = last
        for x in inner + outer:
            if x == outer[0]:
                with scope("halo_last_x"):
                    recv_x(k)
            for r, n in chunks:
                rows = pl.ds(r, n)
                if x in inner:
                    back = state[0, x + 1, rows, :]
                    back = jnp.where(at_lane(x, n), back + zed[rows, pl.ds(0, LANES)], back)
                    back = jnp.where(at_lane(x - 1, n), back + zed[rows, pl.ds(LANES, LANES)], back)
                else:
                    back = adjoint(k, x, r, n)
                v = grad[x, rows, :] + pltpu.roll(back, (LANES - x) % LANES, 1)
                grad[x, rows, :] = v
                total = total + squared(v, r, n)
        acc[...] = total

    @pl.when((t == XS - 1) | (t == XS))
    def _():
        add_earlier()

    for on, ref in ((t == 0, forc), (t == last_t, grad)):
        @pl.when(on)
        def _():
            total = acc[...]
            for x in range(NP):
                for r, n in chunks:
                    total = total + squared(ref[x, pl.ds(r, n), :], r, n)
            acc[...] = total

    stage_a[0] = jnp.sum(acc[...], axis=0, keepdims=True)
    for i, p in enumerate(group_a):
        rdma(stage_a.at[0], stage_a.at[i + 1], p_send.at[0], p_recv.at[0], **peer_a(*p)).start()
    everyone = stage_a.at[pl.ds(1, len(group_a))]
    with scope("sum_a"):
        wait(everyone, p_recv.at[0])
    stage_b[0] = jnp.sum(stage_a[...], axis=0)
    for i, p in enumerate(group_b):
        rdma(stage_b.at[0], stage_b.at[i + 1], p_send.at[1], p_recv.at[1], **peer_b(*p)).start()
    everyone_b = stage_b.at[pl.ds(1, len(group_b))]

    wait(everyone, p_send.at[0])

    @pl.when(runs)
    def _():
        for k in range(2 * STEPS):
            each(halo_copies(k), lambda c: c.wait_send())
        each(coef_copies, lambda c: c.wait_send())
        wait(end.at[:, valid, :], e_send.at[0])

    @pl.when(t > 0)
    def _():
        wait(dual.at[:, valid, :], d_send.at[0])

    @pl.when(t == last_t)
    def _():
        wait(later.at[pl.ds(0, 2 * len(d_round)), valid, :], d_send.at[1])

    @pl.when(t == helper)
    def _():
        wait(side.at[pl.ds(0, 2 * len(d_side)), valid, :], d_send.at[1])

    @pl.when((t == 0) & straight)
    def _():
        wait(earlier.at[:, valid, :], e_send.at[1])

    with scope("sum_b"):
        wait(everyone_b, p_recv.at[1])
    sums[...] = jnp.sum(stage_b[...], axis=0)
    wait(everyone_b, p_send.at[1])


def finish(sz, forc, grad, dual, inc, sums, out_dual, out_incr, done, sem):
    chunks = [(r, min(48, sz.rows - r)) for r in range(0, sz.rows, 48)]
    valid = pl.ds(0, sz.levels)
    global_sum = jnp.sum(sums[...], keepdims=True)
    count = 2 * sz.levels * sz.planes * LANES * sz.tm * sz.gx * sz.gy
    root_mean = jnp.sqrt(global_sum / count + 1e-06)
    scale = jnp.minimum(1.0, 0.5 / root_mean)
    outs = (out_dual, out_incr)
    for x in range(sz.planes):
        for i, (base, step) in enumerate(((dual, forc), (inc, grad))):
            for r, n in chunks:
                rows = pl.ds(r, n)
                done[i, x, rows, :] = base[x, rows, :] + scale * step[x, rows, :]
            pltpu.make_async_copy(done.at[i, x, valid, :], outs[i].at[0, :, x, :], sem.at[i]).start()
    for i in range(2):
        whole = done.at[i, :, valid, :]
        pltpu.make_async_copy(whole, whole, sem.at[i]).wait()


def solution(mesh):
    def local(increment, dual_state, forcing, gradient, courant_x, courant_y, error_var, obs_weight, diffusion, level_mix):
        _, levels, planes, lanes = increment.shape
        assert lanes == LANES
        sz = Sizes(mesh, levels, planes)
        R = sz.rows
        field = pltpu.VMEM((planes, R, LANES), F32)
        plane = pltpu.VMEM((R, LANES), F32)
        n = 2 * STEPS
        thin = 8 * -(-R * planes // (8 * LANES))
        slim = pltpu.VMEM((thin, LANES), F32)
        dma = pltpu.SemaphoreType.DMA
        any_spec = pl.BlockSpec(memory_space=pltpu.HBM)
        vmem_spec = pl.BlockSpec(memory_space=pltpu.VMEM)
        block = jax.ShapeDtypeStruct(increment.shape, F32)
        kept = pl.pallas_call(
            functools.partial(kernel, sz),
            name="saddle",
            out_shape=[pltpu.VMEM((planes, R, LANES), F32)] * 4 + [pltpu.VMEM((1, LANES), F32)],
            in_specs=[any_spec] * 10,
            out_specs=[pl.BlockSpec(memory_space=pltpu.VMEM)] * 5,
            scratch_shapes=[field] * 7
            + [
                pltpu.VMEM((planes // 2, R, LANES), F32),
                pltpu.VMEM((8, LANES), F32),
                pltpu.VMEM((2, R, LANES), F32),
                pltpu.VMEM((R, 2 * LANES), F32),
                plane,
                pltpu.VMEM((planes + 1, R, LANES), F32),
                field,
                field,
                plane,
                pltpu.VMEM((n, planes + 2, R, LANES), F32),
                pltpu.VMEM((n, 2, thin, LANES), F32),
                pltpu.VMEM((n, 2, thin, LANES), F32),
                pltpu.VMEM((2, R, LANES), F32),
                pltpu.VMEM((n, 2, R, LANES), F32),
                slim,
                slim,
                plane,
                plane,
                pltpu.VMEM((1, levels), F32),
                pltpu.VMEM((levels, levels), F32),
                pltpu.VMEM((2, R, sz.depth), BF16),
                pltpu.VMEM((planes // 2 + 1, sz.depth, 2 * LANES), BF16),
                pltpu.VMEM((sz.xs * sz.gy * 2, 1, LANES), F32),
                pltpu.VMEM((sz.gx, 1, LANES), F32),
                dma((10,)),
                dma((2,)),
                dma((planes // 2,)),
                dma((planes // 2,)),
                dma((2,)),
                dma((planes // 2,)),
                dma((n, 4)),
                dma((n, 4)),
                dma((2,)),
                dma((2,)),
                dma((2,)),
                dma((2,)),
            ],
            compiler_params=pltpu.CompilerParams(
                collective_id=0, has_side_effects=True, vmem_limit_bytes=60_000_000
            ),
        )(
            increment, dual_state, forcing, gradient, courant_x, courant_y, error_var, obs_weight,
            diffusion.reshape(1, -1), level_mix,
        )
        return pl.pallas_call(
            functools.partial(finish, sz),
            name="finish",
            out_shape=[block, block],
            in_specs=[vmem_spec] * 5,
            out_specs=[any_spec] * 2,
            scratch_shapes=[pltpu.VMEM((2, planes, R, LANES), F32), dma((2,))],
            compiler_params=pltpu.CompilerParams(vmem_limit_bytes=6_000_000),
        )(*kept)

    spec = P("tm", None, "gx", "gy")
    return jax.shard_map(
        local,
        mesh=mesh,
        in_specs=(spec,) * 8 + (P(), P()),
        out_specs=(spec, spec),
        check_vma=False,
    )
```

```python
import functools

import jax
import jax.numpy as jnp
from jax import lax
from jax.experimental import pallas as pl
from jax.experimental.pallas import tpu as pltpu
from jax.sharding import PartitionSpec as P

STEPS = 3
F32 = jnp.float32
BF16 = jnp.bfloat16
LANES = 128
MESH = pl.DeviceIdType.MESH


class Sizes:
    def __init__(self, mesh, levels, planes):
        self.tm, self.gx, self.gy = (mesh.shape[a] for a in ("tm", "gx", "gy"))
        self.xs = self.tm // 2
        self.levels = levels
        self.planes = planes
        self.rows = -(-levels // 16) * 16
        self.depth = 3 * self.rows


def kernel(
    sz,
    inc_h, dual_h, forc_h, grad_h, cx_h, cy_h, ev_h, ob_h, diff_h, mix_h,
    forc, grad, dual, inc, sums,
    cx, cy, ev, ob,
    later, earlier, end, side, acc, cols, zed, bown,
    ca, cb, cc, sb, state, slim_out, slim_in, edges, xsend, bslim_out, bslim_in, bhalo, asend,
    diff_r, mix_r, wcat, tb, stage_a, stage_b,
    load_sem, d_send, d_recv, s_recv, e_send, e_recv, h_send, h_recv, c_send, c_recv, p_send, p_recv,
):
    NP, R, L = sz.planes, sz.rows, sz.levels
    XS = sz.xs
    t, g, y = (lax.axis_index(a) for a in ("tm", "gx", "gy"))
    xc, zh = lax.rem(t, XS), lax.div(t, XS)
    core, zl = lax.rem(g, 2), lax.div(g, 2)
    last_t = sz.tm - 1
    zchips = sz.gx // 2
    half = NP // 2
    helper = XS + 2
    scope = jax.named_scope

    def rdma(src, dst, ssem, rsem, **where):
        return pltpu.make_async_remote_copy(
            src_ref=src, dst_ref=dst, send_sem=ssem, recv_sem=rsem, device_id=where, device_id_type=MESH
        )

    def wait(ref, sem):
        pltpu.make_async_copy(ref, ref, sem).wait()

    barrier = pltpu.get_barrier_semaphore()
    group_a = [(dx, dy, dc) for dx in range(XS) for dy in range(sz.gy) for dc in range(2)][1:]
    group_b = [(dh, dl) for dh in range(2) for dl in range(zchips)][1:]

    def hops(p):
        return min(p[0], XS - p[0]) + min(p[1], sz.gy - p[1]) + 0.5 * p[2]

    group_a.sort(key=hops, reverse=True)
    group_b.sort(key=lambda p: -p[0])

    def peer_a(dx, dy, dc):
        return {
            "tm": zh * XS + lax.rem(xc + dx, XS),
            "gy": lax.rem(y + dy, sz.gy),
            "gx": zl * 2 + lax.rem(core + dc, 2),
        }

    def peer_b(dh, dl):
        return {"tm": lax.rem(zh + dh, 2) * XS + xc, "gx": lax.rem(zl + dl, zchips) * 2 + core}

    def greet(where):
        pl.semaphore_signal(barrier, inc=1, device_id=where, device_id_type=MESH)

    for p in group_b:
        greet(peer_b(*p))
    for p in group_a:
        greet(peer_a(*p))
    outward = jnp.where(core == 0, g - 1, g + 1)
    has_out = (outward >= 0) & (outward < sz.gx)

    @pl.when(has_out)
    def _():
        greet({"gx": outward})

    other = zl * 2 + 1 - core
    across = jnp.where((t == XS - 1) | (t == XS), 2, jnp.where((t == 0) | (t == helper), 1, 0))

    @pl.when((t == 0) | (t == XS))
    def _():
        greet({"tm": XS - t, "gx": other})

    @pl.when(t == XS - 1)
    def _():
        greet({"tm": XS})
        greet({"tm": helper})

    @pl.when((t == XS) | (t == helper))
    def _():
        greet({"tm": XS - 1})

    hbm = (inc_h, cx_h, cy_h, dual_h, forc_h, ev_h, ob_h, grad_h)
    local = (inc, cx, cy, dual, forc, ev, ob, grad)
    valid = pl.ds(0, L)

    def load(i):
        for x in range(NP):
            pltpu.make_async_copy(hbm[i].at[0, :, x, :], local[i].at[x, valid, :], load_sem.at[i]).start()

    def loaded(i):
        wait(local[i].at[:, valid, :], load_sem.at[i])

    diff_copy = pltpu.make_async_copy(diff_h, diff_r, load_sem.at[8])
    mix_copy = pltpu.make_async_copy(mix_h, mix_r, load_sem.at[9])
    diff_copy.start()
    for i in range(4):
        load(i)
    mix_copy.start()

    lane = lax.broadcasted_iota(jnp.int32, (8, LANES), 1)

    def at_lane(k, n):
        return jnp.broadcast_to((lane == k % LANES)[None], (n // 8, 8, LANES)).reshape(n, LANES)

    chunks = [(r, min(48, R - r)) for r in range(0, R, 48)]

    diff_copy.wait()
    lifted = jnp.concatenate([diff_r[...], jnp.zeros((1, 2 * LANES - L), F32)], axis=1)
    turned = jnp.broadcast_to(lifted, (LANES, 2 * LANES)).T
    sb[...] = turned[:R]

    def widen(m):
        high = m.astype(BF16).astype(F32)
        low = m - high
        tail = jnp.where(lane[:1] < R - LANES, high[:, LANES:], 0.0)
        tail_low = jnp.where(lane[:1] < R - LANES, low[:, LANES:], 0.0)
        k = R - LANES
        tails = tail + pltpu.roll(tail, k, 1) + pltpu.roll(tail_low, 2 * k, 1)
        whole = jnp.concatenate([high[:, :LANES], high[:, :LANES], low[:, :LANES], tails], axis=1)
        return whole[:, : sz.depth].astype(BF16)

    row = lax.broadcasted_iota(jnp.int32, (R, LANES), 0)

    def clean(v, r, n):
        return v if r + n <= L else jnp.where(row[r : r + n] < L, v, 0.0)

    @pl.when(g == 0)
    def _():
        for k in range(2 * STEPS):
            state[k, 0] = jnp.zeros((R, LANES), F32)
        ca[0] = jnp.zeros((R, LANES), F32)

    @pl.when(g == sz.gx - 1)
    def _():
        for k in range(2 * STEPS):
            state[k, NP + 1] = jnp.zeros((R, LANES), F32)

    @pl.when(y == 0)
    def _():
        for k in range(2 * STEPS):
            slim_in[k, 0] = jnp.zeros(slim_in.shape[2:], F32)
        bslim_in[...] = jnp.zeros(bslim_in.shape, F32)

    @pl.when(y == sz.gy - 1)
    def _():
        for k in range(2 * STEPS):
            slim_in[k, 1] = jnp.zeros(slim_in.shape[2:], F32)

    share = LANES // NP

    def slim_tiles(tile, dst, e):
        for o in range(0, R // 8, share):
            acc = tile(pl.ds(8 * o, 8))
            for j in range(1, min(share, R // 8 - o)):
                turned = pltpu.roll(tile(pl.ds(8 * (o + j), 8)), NP * j, 1)
                inside = (lane >= NP * j + e - 1) & (lane < NP * (j + 1) + e - 1)
                acc = jnp.where(inside, turned, acc)
            dst[pl.ds(8 * (o // share), 8), :] = acc

    def slim(planes, dst, sides):
        for e in sides:
            def tile(rows):
                part = planes(0, rows)
                for x in range(1, NP):
                    part = jnp.where(lane == x + e - 1, planes(x, rows), part)
                return part

            slim_tiles(tile, dst(e), e)

    def unslim(src, i):
        tile = src[pl.ds(8 * (i // share), 8), :]
        j = i % share
        return pltpu.roll(tile, LANES - NP * j, 1) if j else tile

    def keep(k, x, r, n, v):
        rows = pl.ds(r, n)
        state[k, x + 1, rows, :] = v
        if x == 0:
            xsend[k, 0, rows, :] = pltpu.roll(v, NP, 1)
        if x == NP - 1:
            xsend[k, 1, rows, :] = pltpu.roll(v, LANES - NP, 1)

    def halo_copies(k):
        return (
            (g > 0, xsend.at[k, 0], state.at[k, NP + 1], h_send.at[k, 0], h_recv.at[k, 0], {"gx": g - 1}),
            (g < sz.gx - 1, xsend.at[k, 1], state.at[k, 0], h_send.at[k, 1], h_recv.at[k, 1], {"gx": g + 1}),
            (y < sz.gy - 1, slim_out.at[k, 0], slim_in.at[k, 0], h_send.at[k, 2], h_recv.at[k, 2], {"gy": y + 1}),
            (y > 0, slim_out.at[k, 1], slim_in.at[k, 1], h_send.at[k, 3], h_recv.at[k, 3], {"gy": y - 1}),
        )

    def each(copies, act):
        for on, src, dst, ssem, rsem, where in copies:
            @pl.when(on)
            def _():
                act(rdma(src, dst, ssem, rsem, **where))

    def send_x(k):
        each(halo_copies(k)[:2], lambda c: c.start())

    def send_y(k):
        slim(lambda x, rows: state[k, x + 1, rows, :], lambda side: slim_out.at[k, side], (0, 1))
        each(halo_copies(k)[2:], lambda c: c.start())

    def recv_x(k):
        for on, ref, i in ((g < sz.gx - 1, state.at[k, NP + 1], 0), (g > 0, state.at[k, 0], 1)):
            @pl.when(on)
            def _():
                wait(ref, h_recv.at[k, i])

    def recv_y(k):
        for on, ref, i in ((y > 0, slim_in.at[k, 0], 2), (y < sz.gy - 1, slim_in.at[k, 1], 3)):
            @pl.when(on)
            def _():
                wait(ref, h_recv.at[k, i])
        for i in range(R // 8):
            rows = pl.ds(8 * i, 8)
            low = unslim(slim_in.at[k, 0], i)
            edges[0, rows, :] = bhalo[rows, :] * low if k < STEPS else low
            edges[1, rows, :] = unslim(slim_in.at[k, 1], i)

    coef_copies = (
        (g < sz.gx - 1, asend, ca.at[0], c_send.at[0], c_recv.at[0], {"gx": g + 1}),
        (y < sz.gy - 1, bslim_out, bslim_in, c_send.at[1], c_recv.at[1], {"gy": y + 1}),
    )
    runs = t != last_t
    def turned_field(ref, x, r, n):
        return pltpu.roll(ref[x, pl.ds(r, n), :], x, 1)

    loaded(0)

    @pl.when(runs)
    def _():
        for x in range(NP):
            for r, n in chunks:
                keep(0, x, r, n, clean(turned_field(inc, x, r, n), r, n))
        slim(lambda x, rows: state[0, x + 1, rows, :], lambda side: slim_out.at[0, side], (0, 1))

    loaded(1)
    loaded(2)

    @pl.when(runs)
    def _():
        for x in range(NP):
            for r, n in chunks:
                rows = pl.ds(r, n)
                cb[x, rows, :] = clean(turned_field(cy, x, r, n) + sb[rows, :], r, n)
        slim(lambda x, rows: cb[x, rows, :], lambda side: bslim_out, (0,))
        for r, n in chunks:
            rows = pl.ds(r, n)
            a = clean(turned_field(cx, NP - 1, r, n) + sb[rows, :], r, n)
            asend[rows, :] = pltpu.roll(a, LANES - NP, 1)

    loaded(3)
    with scope("wait_barrier"):
        pl.semaphore_wait(barrier, len(group_a) + len(group_b) + has_out.astype(jnp.int32) + across)

    @pl.when(runs)
    def _():
        send_x(0)
        each(halo_copies(0)[2:], lambda c: c.start())
        each(coef_copies, lambda c: c.start())

    late = half - 1
    d_order = [0, late] + list(range(1, late))
    third = half // 4 + 1
    d_round, d_side, d_straight = d_order[:third], d_order[third : 2 * third], d_order[2 * third :]
    e_order = list(range(1, late)) + [0, late]
    straight = core == lax.rem(zl, 2)
    around = (t == XS - 1) & jnp.logical_not(straight)

    def pair_of(ref, p):
        return ref.at[pl.ds(2 * p, 2), valid, :]

    def d_copy(p):
        to = jnp.where(t == XS, last_t, t - 1) if p in d_round else t - 1
        return rdma(pair_of(dual, p), pair_of(later, p), d_send.at[0], d_recv.at[p], tm=to)

    def d_pass(p):
        return rdma(pair_of(later, p), pair_of(later, p), d_send.at[1], d_recv.at[p], tm=XS - 1)

    def s_copy(i):
        return rdma(pair_of(dual, d_side[i]), pair_of(side, i), d_send.at[0], s_recv.at[i], tm=helper)

    def s_pass(i):
        p = d_side[i]
        return rdma(pair_of(side, i), pair_of(later, p), d_send.at[1], d_recv.at[p], tm=XS - 1)

    @pl.when(t > 0)
    def _():
        for p in d_round:
            d_copy(p).start()

    @pl.when(t == XS)
    def _():
        for i in range(len(d_side)):
            s_copy(i).start()

    @pl.when((t > 0) & (t != XS))
    def _():
        for p in d_side + d_straight:
            d_copy(p).start()

    for i in range(4, 8):
        load(i)

    @pl.when(t == last_t)
    def _():
        for p in d_round:
            with scope(f"relay_d{p}"):
                wait(pair_of(later, p), d_recv.at[p])
            d_pass(p).start()

    @pl.when(runs)
    def _():
        for x in range(NP):
            for r, n in chunks:
                rows = pl.ds(r, n)
                s = sb[rows, :]
                a = clean(turned_field(cx, x, r, n) + s, r, n)
                ca[x + 1, rows, :] = a
                cc[x, rows, :] = 1.0 - 2.0 * s - a - cb[x, rows, :]

    mix_copy.wait()
    mix = jnp.concatenate([mix_r[...], jnp.zeros((L, 2 * LANES - L), F32)], axis=1)
    mix = jnp.concatenate([mix, jnp.zeros((2 * LANES - L, 2 * LANES), F32)], axis=0)
    wcat[0] = widen(mix[:R])
    wcat[1] = widen(mix.T[:R])

    def mixed(which, pair, emit):
        out = jnp.dot(wcat[which], tb[pair], preferred_element_type=F32)
        for j in range(2):
            for r, n in chunks:
                emit(2 * pair + j, r, n, out[r : r + n, j * LANES : (j + 1) * LANES])

    def put(pair, j, r, n, v):
        high = v.astype(BF16)
        low = (v - high.astype(F32)).astype(BF16)
        cols = pl.ds(j * LANES, LANES)
        tail = R - LANES
        main = min(n, LANES - r)
        if main > 0:
            tb[pair, pl.ds(r, main), cols] = high[:main]
            tb[pair, pl.ds(LANES + r, main), cols] = low[:main]
            tb[pair, pl.ds(2 * LANES + r, main), cols] = high[:main]
        if main < n:
            m = max(main, 0)
            o = 3 * LANES + r + m - LANES
            tb[pair, pl.ds(o, n - m), cols] = high[m:]
            tb[pair, pl.ds(o + tail, n - m), cols] = low[m:]
            tb[pair, pl.ds(o + 2 * tail, n - m), cols] = high[m:]

    def edge_of(side, rows, edge):
        return edges[side, rows, :] if edge else 0.0

    def tangent(k, x, r, n, edge=True):
        rows = pl.ds(r, n)
        v = state[k, x + 1, rows, :]
        from_low = ca[x, rows, :] * state[k, x, rows, :] + jnp.where(
            at_lane(x - 1, n), edge_of(0, rows, edge), cb[x, rows, :] * v
        )
        from_high = state[k, x + 2, rows, :] + jnp.where(at_lane(x, n), edge_of(1, rows, edge), v)
        return cc[x, rows, :] * v + pltpu.roll(from_low, 1, 1) + sb[rows, :] * pltpu.roll(from_high, LANES - 1, 1)

    def adjoint(k, x, r, n, edge=True):
        rows = pl.ds(r, n)
        w = state[k, x + 1, rows, :]
        low = state[k, x, rows, :] + jnp.where(at_lane(x - 1, n), edge_of(0, rows, edge), w)
        up_x = pltpu.roll(state[k, x + 2, rows, :], LANES - 1, 1)
        up_y = pltpu.roll(jnp.where(at_lane(x, n), edge_of(1, rows, edge), w), LANES - 1, 1)
        out = cc[x, rows, :] * w + ca[x + 1, rows, :] * up_x + cb[x, rows, :] * up_y
        return out + sb[rows, :] * pltpu.roll(low, 1, 1)

    def tangent_edges(rows):
        first = pltpu.roll(edges[0, rows, :], 1, 1)
        return first, sb[rows, :] * pltpu.roll(edges[1, rows, :], LANES - 1, 1)

    def adjoint_edges(rows):
        first = sb[rows, :] * pltpu.roll(edges[0, rows, :], 1, 1)
        return first, bown[rows, :] * pltpu.roll(edges[1, rows, :], LANES - 1, 1)

    inner_pairs, outer_pairs = list(range(1, half - 1)), [0, half - 1]
    inner = list(range(2, NP - 2))
    outer = [0, 1, NP - 2, NP - 1]

    def step_inner(k, which, stencil, emit):
        for pair in inner_pairs:
            for j in range(2):
                for r, n in chunks:
                    put(pair, j, r, n, stencil(k, 2 * pair + j, r, n, False))
            mixed(which, pair, emit)

    def step_edges(which, stencil_edges):
        for r, n in chunks:
            for j, v in enumerate(stencil_edges(pl.ds(r, n))):
                put(half, j, r, n, v)
        zed[...] = jnp.dot(wcat[which], tb[half], preferred_element_type=F32)

    def step_outer(k, which, stencil, emit):
        for pair in outer_pairs:
            for j in range(2):
                for r, n in chunks:
                    put(pair, j, r, n, stencil(k, 2 * pair + j, r, n))
            mixed(which, pair, emit)

    def advance(k, which, stencil, stencil_edges, extra_y, extra_x, after):
        emit = functools.partial(keep, k + 1)
        step_inner(k, which, stencil, emit)
        for i in range(R // 8):
            rows = pl.ds(8 * i, 8)
            part = [None, None]
            for x in inner:
                v = state[k + 1, x + 1, rows, :]
                for e in range(2):
                    part[e] = v if part[e] is None else jnp.where(lane == x + e - 1, v, part[e])
            for e in range(2):
                cols[e, rows, :] = part[e]
        with scope(f"halo_y{k}"):
            extra_y()
            recv_y(k)
        with scope(f"halo_x{k}"):
            extra_x()
            recv_x(k)
        step_edges(which, stencil_edges)
        step_outer(k, which, stencil, emit)
        send_x(k + 1)
        for i in range(R // 8):
            rows = pl.ds(8 * i, 8)
            for e in range(2):
                v = cols[e, rows, :] + zed[rows, pl.ds((1 - e) * LANES, LANES)]
                for x in outer:
                    v = jnp.where(lane == (x + e - 1) % LANES, state[k + 1, x + 1, rows, :], v)
                cols[e, rows, :] = v
        for e in range(2):
            slim_tiles(lambda rows: cols[e, rows, :], slim_out.at[k + 1, e], e)
        each(halo_copies(k + 1)[2:], lambda c: c.start())
        after()
        for x in inner:
            for e in range(2):
                pltpu.store(state.at[k + 1, x + 1], cols[e], mask=at_lane(x + e - 1, R))

    def e_copy(p):
        to, column = jnp.where(around, 0, t + 1), jnp.where(around, other, g)
        return rdma(pair_of(end, p), pair_of(earlier, p), e_send.at[0], e_recv.at[p], tm=to, gx=column)

    def e_pass(p):
        return rdma(pair_of(earlier, p), pair_of(earlier, p), e_send.at[1], e_recv.at[p], tm=XS, gx=other)

    def keep_end(x, r, n, v):
        end[x, pl.ds(r, n), :] = pltpu.roll(v, (LANES - x) % LANES, 1)

    def nothing():
        pass

    def first_y():
        @pl.when(y > 0)
        def _():
            wait(bslim_in, c_recv.at[1])
        for i in range(R // 8):
            bhalo[pl.ds(8 * i, 8), :] = unslim(bslim_in, i)

    def first_x():
        @pl.when(g > 0)
        def _():
            wait(ca.at[0], c_recv.at[0])

    def cross():
        @pl.when(t == XS)
        def _():
            for p in d_straight:
                d_copy(p).start()

        @pl.when(t == helper)
        def _():
            for i in range(len(d_side)):
                with scope(f"side{i}"):
                    wait(pair_of(side, i), s_recv.at[i])
                s_pass(i).start()

    def keep_turned(x, r, n, v):
        end[x, pl.ds(r, n), :] = v

    @pl.when(runs)
    def _():
        for k in range(STEPS - 1):
            advance(
                k, 0, tangent, tangent_edges,
                nothing if k else first_y, nothing if k else first_x, cross if k == STEPS - 2 else nothing,
            )
        k = STEPS - 1
        step_inner(k, 0, tangent, keep_turned)
        for i in range(R // 8):
            bown[pl.ds(8 * i, 8), :] = unslim(bslim_out, i)
        with scope(f"halo_y{k}"):
            recv_y(k)
        step_edges(0, tangent_edges)
        for i, pair in enumerate(inner_pairs):
            for x in (2 * pair, 2 * pair + 1):
                for r, n in chunks:
                    rows = pl.ds(r, n)
                    v = end[x, rows, :]
                    v = jnp.where(at_lane(x, n), v + zed[rows, pl.ds(0, LANES)], v)
                    v = jnp.where(at_lane(x - 1, n), v + zed[rows, pl.ds(LANES, LANES)], v)
                    keep_end(x, r, n, v)
            if i == 1:
                for p in e_order[:2]:
                    e_copy(p).start()
        with scope(f"halo_x{k}"):
            recv_x(k)
        step_outer(k, 0, tangent, keep_end)
        for p in e_order[2:]:
            e_copy(p).start()

    for i in range(4, 8):
        loaded(i)
    for x in range(NP):
        for r, n in chunks:
            rows = pl.ds(r, n)
            forc[x, rows, :] = forc[x, rows, :] - ev[x, rows, :] * dual[x, rows, :] - inc[x, rows, :]
            grad[x, rows, :] = grad[x, rows, :] - ob[x, rows, :] * inc[x, rows, :] - dual[x, rows, :]

    @pl.when(runs)
    def _():
        k = STEPS
        for i, pair in enumerate(d_order):
            @pl.when((t == 0) & straight)
            def _():
                p = e_order[i]
                with scope(f"relay_e{p}"):
                    wait(pair_of(earlier, p), e_recv.at[p])
                e_pass(p).start()

            with scope(f"wait_d{pair}"):
                wait(pair_of(later, pair), d_recv.at[pair])
            for j in range(2):
                x = 2 * pair + j
                for r, n in chunks:
                    put(pair, j, r, n, clean(turned_field(later, x, r, n), r, n))
            mixed(1, pair, functools.partial(keep, k))
            if i == 1:
                send_x(k)
        send_y(k)
        for k in range(STEPS, 2 * STEPS - 1):
            advance(k, 1, adjoint, adjoint_edges, nothing, nothing, nothing)
        for x in inner:
            for r, n in chunks:
                state[0, x + 1, pl.ds(r, n), :] = adjoint(2 * STEPS - 1, x, r, n, False)

    def squared(v, r, n):
        v = clean(v, r, n)
        return jnp.sum((v * v).reshape(n // 8, 8, LANES), axis=0)

    def add_earlier():
        total = acc[...]
        for p in e_order:
            with scope(f"wait_e{p}"):
                wait(pair_of(earlier, p), e_recv.at[p])
            for x in (2 * p, 2 * p + 1):
                for r, n in chunks:
                    rows = pl.ds(r, n)
                    v = forc[x, rows, :] + earlier[x, rows, :]
                    forc[x, rows, :] = v
                    total = total + squared(v, r, n)
        acc[...] = total

    acc[...] = jnp.zeros((8, LANES), F32)

    @pl.when((t > 0) & (t != XS - 1) & (t != XS))
    def _():
        add_earlier()

    @pl.when(runs)
    def _():
        k = 2 * STEPS - 1
        with scope("halo_last"):
            recv_y(k)
        total = acc[...]
        for r, n in chunks:
            rows = pl.ds(r, n)
            first, last = adjoint_edges(rows)
            zed[rows, pl.ds(0, LANES)] = first
            zed[rows, pl.ds(LANES, LANES)] = last
        for x in inner + outer:
            if x == outer[0]:
                with scope("halo_last_x"):
                    recv_x(k)
            for r, n in chunks:
                rows = pl.ds(r, n)
                if x in inner:
                    back = state[0, x + 1, rows, :]
                    back = jnp.where(at_lane(x, n), back + zed[rows, pl.ds(0, LANES)], back)
                    back = jnp.where(at_lane(x - 1, n), back + zed[rows, pl.ds(LANES, LANES)], back)
                else:
                    back = adjoint(k, x, r, n)
                v = grad[x, rows, :] + pltpu.roll(back, (LANES - x) % LANES, 1)
                grad[x, rows, :] = v
                total = total + squared(v, r, n)
        acc[...] = total

    @pl.when((t == XS - 1) | (t == XS))
    def _():
        add_earlier()

    for on, ref in ((t == 0, forc), (t == last_t, grad)):
        @pl.when(on)
        def _():
            total = acc[...]
            for x in range(NP):
                for r, n in chunks:
                    total = total + squared(ref[x, pl.ds(r, n), :], r, n)
            acc[...] = total

    stage_a[0] = jnp.sum(acc[...], axis=0, keepdims=True)
    for i, p in enumerate(group_a):
        rdma(stage_a.at[0], stage_a.at[i + 1], p_send.at[0], p_recv.at[0], **peer_a(*p)).start()
    everyone = stage_a.at[pl.ds(1, len(group_a))]
    with scope("sum_a"):
        wait(everyone, p_recv.at[0])
    stage_b[0] = jnp.sum(stage_a[...], axis=0)
    for i, p in enumerate(group_b):
        rdma(stage_b.at[0], stage_b.at[i + 1], p_send.at[1], p_recv.at[1], **peer_b(*p)).start()
    everyone_b = stage_b.at[pl.ds(1, len(group_b))]

    wait(everyone, p_send.at[0])

    @pl.when(runs)
    def _():
        for k in range(2 * STEPS):
            each(halo_copies(k), lambda c: c.wait_send())
        each(coef_copies, lambda c: c.wait_send())
        wait(end.at[:, valid, :], e_send.at[0])

    @pl.when(t > 0)
    def _():
        wait(dual.at[:, valid, :], d_send.at[0])

    @pl.when(t == last_t)
    def _():
        wait(later.at[pl.ds(0, 2 * len(d_round)), valid, :], d_send.at[1])

    @pl.when(t == helper)
    def _():
        wait(side.at[pl.ds(0, 2 * len(d_side)), valid, :], d_send.at[1])

    @pl.when((t == 0) & straight)
    def _():
        wait(earlier.at[:, valid, :], e_send.at[1])

    with scope("sum_b"):
        wait(everyone_b, p_recv.at[1])
    sums[...] = jnp.sum(stage_b[...], axis=0)
    wait(everyone_b, p_send.at[1])


def finish(sz, forc, grad, dual, inc, sums, out_dual, out_incr, done, sem):
    chunks = [(r, min(48, sz.rows - r)) for r in range(0, sz.rows, 48)]
    valid = pl.ds(0, sz.levels)
    global_sum = jnp.sum(sums[...], keepdims=True)
    count = 2 * sz.levels * sz.planes * LANES * sz.tm * sz.gx * sz.gy
    root_mean = jnp.sqrt(global_sum / count + 1e-06)
    scale = jnp.minimum(1.0, 0.5 / root_mean)
    outs = (out_dual, out_incr)
    for x in range(sz.planes):
        for i, (base, step) in enumerate(((dual, forc), (inc, grad))):
            for r, n in chunks:
                rows = pl.ds(r, n)
                done[i, x, rows, :] = base[x, rows, :] + scale * step[x, rows, :]
            pltpu.make_async_copy(done.at[i, x, valid, :], outs[i].at[0, :, x, :], sem.at[i]).start()
    for i in range(2):
        whole = done.at[i, :, valid, :]
        pltpu.make_async_copy(whole, whole, sem.at[i]).wait()


def solution(mesh):
    def local(increment, dual_state, forcing, gradient, courant_x, courant_y, error_var, obs_weight, diffusion, level_mix):
        _, levels, planes, lanes = increment.shape
        assert lanes == LANES
        sz = Sizes(mesh, levels, planes)
        R = sz.rows
        field = pltpu.VMEM((planes, R, LANES), F32)
        plane = pltpu.VMEM((R, LANES), F32)
        n = 2 * STEPS
        thin = 8 * -(-R * planes // (8 * LANES))
        slim = pltpu.VMEM((thin, LANES), F32)
        dma = pltpu.SemaphoreType.DMA
        any_spec = pl.BlockSpec(memory_space=pltpu.HBM)
        vmem_spec = pl.BlockSpec(memory_space=pltpu.VMEM)
        block = jax.ShapeDtypeStruct(increment.shape, F32)
        kept = pl.pallas_call(
            functools.partial(kernel, sz),
            name="saddle",
            out_shape=[pltpu.VMEM((planes, R, LANES), F32)] * 4 + [pltpu.VMEM((1, LANES), F32)],
            in_specs=[any_spec] * 10,
            out_specs=[pl.BlockSpec(memory_space=pltpu.VMEM)] * 5,
            scratch_shapes=[field] * 7
            + [
                pltpu.VMEM((planes // 2, R, LANES), F32),
                pltpu.VMEM((8, LANES), F32),
                pltpu.VMEM((2, R, LANES), F32),
                pltpu.VMEM((R, 2 * LANES), F32),
                plane,
                pltpu.VMEM((planes + 1, R, LANES), F32),
                field,
                field,
                plane,
                pltpu.VMEM((n, planes + 2, R, LANES), F32),
                pltpu.VMEM((n, 2, thin, LANES), F32),
                pltpu.VMEM((n, 2, thin, LANES), F32),
                pltpu.VMEM((2, R, LANES), F32),
                pltpu.VMEM((n, 2, R, LANES), F32),
                slim,
                slim,
                plane,
                plane,
                pltpu.VMEM((1, levels), F32),
                pltpu.VMEM((levels, levels), F32),
                pltpu.VMEM((2, R, sz.depth), BF16),
                pltpu.VMEM((planes // 2 + 1, sz.depth, 2 * LANES), BF16),
                pltpu.VMEM((sz.xs * sz.gy * 2, 1, LANES), F32),
                pltpu.VMEM((sz.gx, 1, LANES), F32),
                dma((10,)),
                dma((2,)),
                dma((planes // 2,)),
                dma((planes // 2,)),
                dma((2,)),
                dma((planes // 2,)),
                dma((n, 4)),
                dma((n, 4)),
                dma((2,)),
                dma((2,)),
                dma((2,)),
                dma((2,)),
            ],
            compiler_params=pltpu.CompilerParams(
                collective_id=0, has_side_effects=True, vmem_limit_bytes=60_000_000
            ),
        )(
            increment, dual_state, forcing, gradient, courant_x, courant_y, error_var, obs_weight,
            diffusion.reshape(1, -1), level_mix,
        )
        return pl.pallas_call(
            functools.partial(finish, sz),
            name="finish",
            out_shape=[block, block],
            in_specs=[vmem_spec] * 5,
            out_specs=[any_spec] * 2,
            scratch_shapes=[pltpu.VMEM((2, planes, R, LANES), F32), dma((2,))],
            compiler_params=pltpu.CompilerParams(vmem_limit_bytes=6_000_000),
        )(*kept)

    spec = P("tm", None, "gx", "gy")
    return jax.shard_map(
        local,
        mesh=mesh,
        in_specs=(spec,) * 8 + (P(), P()),
        out_specs=(spec, spec),
        check_vma=False,
    )
```
